256 devices in a mesh: gx: 16 (over z, core), gy: 16 (over x, y).
Axes of the slice: x: 4, y: 4, z: 8, core: 2. Of those that a mesh axis runs over, the one named last changes fastest.
Arguments:
- earlier_heat_field: float32 [6, 2048, 2048], P(None, 'gx', 'gy'), may hold values from -6 to 6
- substance_per_voxel: int32 [6, 2048, 2048], P(None, 'gx', 'gy'), may hold values from 0 to 7
- patch_wattage_category: int32 [128, 128], P('gx', 'gy'), may hold values from 0 to 63
- planar_coupling: float32 [8], replicated, may hold values from 0.3 to 3
- vertical_coupling_per_substance: float32 [8], replicated, may hold values from 0.05 to 0.5
- heat_mass_ratio: float32 [8], replicated, may hold values from 2e-05 to 0.0002
- wattage_per_category: float32 [64], replicated, may hold values from 2e-06 to 2e-05
Outputs:
- temperature: float32 [6, 2048, 2048], P(None, 'gx', 'gy')
The draws below stay inside these ranges and needn't reach their ends.
All inputs are finite; a program needn't handle non-finite values.
Results may differ from the reference program's by a relative error of at most 0.0003.
Values sent between devices are 32-bit elements; how exact they have to be, the bound alone decides.
A program may use at most 192 MiB of HBM per device.

```python
import math
import jax
import jax.numpy as jnp
from jax import lax

DIE_COUNT = 6
MATERIALS = 8
POWER_LEVELS = 64
TILE = 16
LEVELS = 6
SWEEPS = 2
COARSE_ITERS = 12
CX = 128
GRID_LENGTH = 2048
GRID_WIDTH = 2048


def draw_substance_per_voxel(key, part):
    block_key = jax.random.fold_in(key, 11)
    noise_key = jax.random.fold_in(key, 23)
    pick_key = jax.random.fold_in(key, 37)
    blocks = jax.random.randint(block_key, (DIE_COUNT, GRID_LENGTH // CX, GRID_WIDTH // CX), 0, MATERIALS)
    spread = jnp.repeat(jnp.repeat(blocks, CX, axis=1), CX, axis=2)
    shape = (DIE_COUNT, GRID_LENGTH, GRID_WIDTH)
    noise = jax.random.randint(noise_key, shape, 0, MATERIALS)
    pick = jax.random.randint(pick_key, shape, 0, 4)
    return jnp.where(pick == 0, noise, spread).astype(jnp.int32)


def plant(values, stream_key, smallest, high):
    dims = values.shape
    place = [jax.random.randint(jax.random.fold_in(stream_key, axis), (), 0, dims[axis]) for axis in range(len(dims))]
    values = values.at[tuple(place)].set(smallest)
    longest = dims.index(max(dims))
    place[longest] = (place[longest] + 1) % dims[longest]
    return values.at[tuple(place)].set(high)


def shard_levels(rng, dims, shards, least, top_value):
    loudness, own = 1.0, jax.random.fold_in(rng, 6)
    for axis_at, blocks in shards:
        draws = jnp.exp(jax.random.uniform(jax.random.fold_in(own, axis_at), (blocks,), jnp.float32, least / len(shards), top_value / len(shards)))
        loudness = loudness * jnp.repeat(draws, dims[axis_at] // blocks).reshape([-1 if axis == axis_at else 1 for axis in range(len(dims))])
    return loudness


def scatter_about(own_key, dims, width, limit, shards=(), held_as=jnp.bfloat16):
    loudness = shard_levels(own_key, dims, shards, -0.22, 0.18) if shards else 1.0
    values = jax.random.normal(own_key, dims, jnp.float32) * width * loudness
    return jnp.minimum(jnp.maximum(values, -limit), limit).astype(held_as)


def setup_inputs(seed: int = 0) -> dict:
    seeds = jax.random.split(jax.random.key(seed), 8)
    return {
        "earlier_heat_field": scatter_about(seeds[0], (DIE_COUNT, GRID_LENGTH, GRID_WIDTH), 1.0, 6.0, ((1, 16), (2, 16)), jnp.float32),
        "substance_per_voxel": draw_substance_per_voxel(jax.random.fold_in(seeds[7], 71), 0),
        "patch_wattage_category": plant(jax.random.randint(seeds[2], (GRID_LENGTH // TILE, GRID_WIDTH // TILE), 0, POWER_LEVELS), jax.random.fold_in(seeds[2], 1), 0, POWER_LEVELS - 1).astype(jnp.int32),
        "planar_coupling": jnp.clip(jnp.exp(jax.random.uniform(seeds[3], (MATERIALS,), jnp.float32, math.log(0.3), math.log(3.0))), 0.3, 3.0),
        "vertical_coupling_per_substance": jnp.clip(jnp.exp(jax.random.uniform(seeds[4], (MATERIALS,), jnp.float32, math.log(0.05), math.log(0.5))), 0.05, 0.5),
        "heat_mass_ratio": jnp.clip(jnp.exp(jax.random.uniform(seeds[5], (MATERIALS,), jnp.float32, math.log(1.9999999494757503e-05), math.log(0.0002))), 1.9999999494757503e-05, 0.0002),
        "wattage_per_category": jnp.clip(jnp.exp(jax.random.uniform(seeds[6], (POWER_LEVELS,), jnp.float32, math.log(1.9999999949504854e-06), math.log(1.9999999494757503e-05))), 1.9999999949504854e-06, 1.9999999494757503e-05),
    }


def previous(values, dimension):
    widths = [(0, 0)] * values.ndim
    widths[dimension] = (1, 0)
    return lax.slice_in_dim(jnp.pad(values, widths), 0, values.shape[dimension], axis=dimension)


def following(values, dimension):
    widths = [(0, 0)] * values.ndim
    widths[dimension] = (0, 1)
    return lax.slice_in_dim(jnp.pad(values, widths), 1, values.shape[dimension] + 1, axis=dimension)


def stencil(lateral, vertical, capacity_diagonal, inside, factor):
    row_before = factor * 0.5 * (lateral + previous(lateral, 1))
    row_after = factor * 0.5 * (lateral + following(lateral, 1))
    col_before = factor * 0.5 * (lateral + previous(lateral, 2))
    col_after = factor * 0.5 * (lateral + following(lateral, 2))
    faces = 0.5 * (vertical[1:] + vertical[:-1])
    no_face = jnp.zeros_like(vertical[:1])
    layer_below = jnp.concatenate([no_face, faces], 0)
    layer_above = jnp.concatenate([faces, no_face], 0)
    diagonal = capacity_diagonal + row_before + row_after + col_before + col_after + layer_below + layer_above
    diagonal = jnp.where(inside > 0, diagonal, 1.0)
    return (row_before, row_after, col_before, col_after, layer_below, layer_above, diagonal)


def coupled(values, weights):
    summed = weights[0] * previous(values, 1) + weights[1] * following(values, 1)
    summed = summed + weights[2] * previous(values, 2) + weights[3] * following(values, 2)
    return summed + weights[4] * previous(values, 0) + weights[5] * following(values, 0)


def parity(extent):
    summed = lax.broadcasted_iota(jnp.int32, extent, 0) + lax.broadcasted_iota(jnp.int32, extent, 1)
    return (summed + lax.broadcasted_iota(jnp.int32, extent, 2)) % 2


def restrict(values):
    layers, height, breadth = values.shape
    blocks = values.reshape(layers, height // 2, 2, breadth // 2, 2)
    return (blocks[:, :, 0, :, 0] + blocks[:, :, 1, :, 0] + blocks[:, :, 0, :, 1] + blocks[:, :, 1, :, 1]) * 0.25


def prolong(values):
    return jnp.repeat(jnp.repeat(values, 2, axis=1), 2, axis=2)


def lookup(labels, entries):
    summed = jnp.zeros(labels.shape, entries.dtype)
    for number in range(entries.shape[0]):
        summed = summed + jnp.where(labels == number, entries[number], 0.0)
    return summed


def conjugate(source_vector, weights):
    solution = jnp.zeros_like(source_vector)
    residue = source_vector
    precond = residue / weights[6]
    search = precond
    inner = jnp.sum(residue * precond)
    for step_index in range(COARSE_ITERS):
        image = weights[6] * search - coupled(search, weights)
        alpha_step = inner / jnp.sum(search * image)
        solution = solution + alpha_step * search
        residue = residue - alpha_step * image
        precond = residue / weights[6]
        inner_next = jnp.sum(residue * precond)
        search = precond + (inner_next / inner) * search
        inner = inner_next
    return solution


def smooth(present_guess, source_vector, weights, colours):
    for sweep_index in range(SWEEPS):
        for colour in (0, 1):
            candidate = (source_vector + coupled(present_guess, weights)) / weights[6]
            present_guess = jnp.where(colours == colour, candidate, present_guess)
    return present_guess


def reference(earlier_heat_field, substance_per_voxel, patch_wattage_category, planar_coupling, vertical_coupling_per_substance, heat_mass_ratio, wattage_per_category):
    lateral = lookup(substance_per_voxel, planar_coupling)
    vertical = lookup(substance_per_voxel, vertical_coupling_per_substance)
    capacity_diagonal = lookup(substance_per_voxel, heat_mass_ratio)
    heat = jnp.repeat(jnp.repeat(lookup(patch_wattage_category, wattage_per_category), TILE, axis=0), TILE, axis=1)
    source_vector = capacity_diagonal * earlier_heat_field
    source_vector = jnp.concatenate([source_vector[:1] + heat[None], source_vector[1:]], 0)
    coefficients = [(lateral, vertical, capacity_diagonal)]
    for level_index in range(LEVELS):
        last = coefficients[-1]
        coefficients.append((restrict(last[0]), restrict(last[1]), restrict(last[2])))
    present_guess = earlier_heat_field
    saved = []
    for level_index in range(LEVELS):
        level_coef = coefficients[level_index]
        weights = stencil(level_coef[0], level_coef[1], level_coef[2], jnp.ones_like(source_vector), 0.25 ** level_index)
        colours = parity(source_vector.shape)
        present_guess = smooth(present_guess, source_vector, weights, colours)
        residual = source_vector - (weights[6] * present_guess - coupled(present_guess, weights))
        saved.append((present_guess, source_vector, weights, colours))
        source_vector = restrict(residual)
        present_guess = jnp.zeros_like(source_vector)
    coarse_coef = coefficients[LEVELS]
    coarse_weights = stencil(coarse_coef[0], coarse_coef[1], coarse_coef[2], jnp.ones_like(source_vector), 0.25 ** LEVELS)
    correction = conjugate(source_vector, coarse_weights)
    for level_index in reversed(range(LEVELS)):
        present_guess, source_vector, weights, colours = saved[level_index]
        present_guess = smooth(present_guess + prolong(correction), source_vector, weights, colours)
        correction = present_guess
    return correction
```

```python
import jax
import jax.numpy as jnp
from jax import lax
from jax.experimental import pallas as pl
from jax.experimental.pallas import tpu as pltpu
from jax.sharding import PartitionSpec as P

MESH = pl.DeviceIdType.MESH
NL = 6
TILE = 16
ITERS = 12
F32 = jnp.float32


class Level:
    def __init__(self, index, block, base, rows, half, whole=False):
        self.index, self.block, self.base, self.rows, self.half, self.whole = index, block, base, rows, half, whole
        self.total = rows + 16
        self.scale = 0.25**index
        step = 24 if rows % 24 == 0 else 16 if rows % 16 == 0 else 8
        self.chunks = [(r, min(step, 8 + rows - r)) for r in range(8, 8 + rows, step)]


def lanes(n):
    return lax.broadcasted_iota(jnp.int32, (n, 128), 1)


def odd(n, k, c):
    bit = lanes(n) & 1
    return bit == 1 if (k + c) % 2 == 0 else bit == 0


def roll(x, shift):
    shift %= 128
    return x if shift == 0 else pltpu.roll(x, shift, 1)


def take(x, index):
    return jnp.take_along_axis(x, index, axis=1, mode="promise_in_bounds")


def thin(x):
    return take(x + roll(x, 127), (2 * lanes(x.shape[0])) & 127)


def wide(x, split=64):
    j = lanes(x.shape[0])
    return take(x, jnp.where(j < split, j >> 1, 64 + (j >> 1)))


def around(refs, t, o, k, r, n, c, pick=()):
    ref = refs[t]
    here = ref[(o, *pick, k, pl.ds(r, n), slice(None))]
    before = ref[(o, *pick, k, pl.ds(r - 1, n), slice(None))]
    after = ref[(o, *pick, k, pl.ds(r + 1, n), slice(None))]
    far = jnp.where(odd(n, k, c), after, before)
    left, right = roll(here, 1), roll(here, 127)
    if len(refs) == 2:
        j = lanes(n)
        beside = refs[1 - t][(o, *pick, k, pl.ds(r, n), slice(None))]
        left = jnp.where(j == 0, roll(beside, 1), left)
        right = jnp.where(j == 127, roll(beside, 127), right)
    return here, far, left, right


def candidate(lv, s, t, c, k, r, n):
    o = 1 - c
    cf = s["cf"][t]
    here, far, left, right = around(s["u"], t, o, k, r, n, c)
    rows = pl.ds(r, n)
    a = cf[c, 0, k, rows, :] * here + cf[c, 1, k, rows, :] * far
    b = cf[c, 2, k, rows, :] * left + cf[c, 3, k, rows, :] * right
    if k > 0:
        a = a + cf[c, 4, k, rows, :] * s["u"][t][o, k - 1, rows, :]
    if k < NL - 1:
        b = b + cf[c, 5, k, rows, :] * s["u"][t][o, k + 1, rows, :]
    return a + b


def half_sweep(lv, s, c):
    for t in range(len(s["u"])):
        for k in range(NL):
            for r, n in lv.chunks:
                rows = pl.ds(r, n)
                s["u"][t][c, k, rows, :] = s["cf"][t][c, 6, k, rows, :] + candidate(lv, s, t, c, k, r, n)


def smooth(lv, s):
    def sweep(i, _):
        half_sweep(lv, s, 0)
        half_sweep(lv, s, 1)
        return 0

    lax.fori_loop(0, 2, sweep, 0)


def residual(lv, s, t, k, r, n):
    rows = pl.ds(r, n)
    parts = []
    for c in (0, 1):
        new = s["cf"][t][c, 6, k, rows, :] + candidate(lv, s, t, c, k, r, n)
        parts.append(s["dg"][t][c, k, rows, :] * (new - s["u"][t][c, k, rows, :]))
    return parts[0] + parts[1]


def inside(lv, t, r, n, gx, gy, nx, ny):
    row = lax.broadcasted_iota(jnp.int32, (n, 128), 0) + (r - lv.base)
    j = lanes(n)
    if lv.whole:
        return (row >= 0) & (row < lv.block * nx // 2) & (j < lv.block * ny)
    half = lv.half // 2
    if lv.index == 0:
        col = j if t == 0 else jnp.where(j < 64, j + 128, j - 128)
    elif lv.index == 1:
        col = jnp.where(j < 96, j, j - 128)
    else:
        col = jnp.where(j < 64, j, j - 128)
    ok = (row >= -half) & (row < lv.block // 2 + half) & (col >= -lv.half) & (col < lv.block + lv.half)
    row, col = row + gx * (lv.block // 2), col + gy * lv.block
    return ok & (row >= 0) & (row < lv.block * nx // 2) & (col >= 0) & (col < lv.block * ny)


def weigh(lv, s, place):
    h = 0.5 * lv.scale
    for t in range(len(s["u"])):
        co = s["co"]
        for r, n in lv.chunks:
            ok = inside(lv, t, r, n, *place)
            rows = pl.ds(r, n)
            for c in (0, 1):
                o = 1 - c
                for k in range(NL):
                    own = co[t][c, 0, k, rows, :]
                    ws = [h * (own + x) for x in around(co, t, o, k, r, n, c, (0,))]
                    diag = co[t][c, 2, k, rows, :] + ((ws[0] + ws[1]) + (ws[2] + ws[3]))
                    mine = co[t][c, 1, k, rows, :]
                    for other, there in ((k - 1, k > 0), (k + 1, k < NL - 1)):
                        if there:
                            face = 0.5 * (mine + co[t][o, 1, other, rows, :])
                            diag = diag + face
                            ws.append(face)
                        else:
                            ws.append(None)
                    inv = jnp.where(ok, 1.0 / diag, 0.0)
                    for i, w in enumerate(ws):
                        if w is not None:
                            s["cf"][t][c, i, k, rows, :] = w * inv
                    s["dg"][t][c, k, rows, :] = diag
                    s["iv"][t][c, k, rows, :] = inv


def pairs(ref, a, start, lv, r, n):
    first = start + 2 * (r - 8)
    even = ref[a, pl.ds(first, n, stride=2), :]
    other = ref[a, pl.ds(first + 1, n, stride=2), :]
    return even, other


def pack_coefficients(lv, s, src, start):
    for m in range(3):
        for k in range(NL):
            for r, n in lv.chunks:
                even, other = pairs(src, m * NL + k, start, lv, r, n)
                for c in (0, 1):
                    s["co"][0][c, m, k, pl.ds(r, n), :] = jnp.where(odd(n, k, c), other, even)


def pack_rhs(lv, s, src, start):
    for k in range(NL):
        for r, n in lv.chunks:
            even, other = pairs(src, k, start, lv, r, n)
            rows = pl.ds(r, n)
            for c in (0, 1):
                f = jnp.where(odd(n, k, c), other, even)
                s["cf"][0][c, 6, k, rows, :] = s["iv"][0][c, k, rows, :] * f


def restrict_rhs(lv, s, dst):
    for k in range(NL):
        for r, n in lv.chunks:
            dst[k, pl.ds(r, n), :] = 0.25 * thin(residual(lv, s, 0, k, r, n))


def restrict_coefficients(lv, s, dst):
    for m in range(3):
        for k in range(NL):
            for r, n in lv.chunks:
                rows = pl.ds(r, n)
                dst[m * NL + k, rows, :] = 0.25 * thin(s["co"][0][0, m, k, rows, :] + s["co"][0][1, m, k, rows, :])


def spread(lv, s, dst):
    for k in range(NL):
        for r, n in lv.chunks:
            red, black = s["u"][0][0, k, pl.ds(r, n), :], s["u"][0][1, k, pl.ds(r, n), :]
            m = odd(n, k, 0)
            dst[k, pl.ds(2 * r, n, stride=2), :] = jnp.where(m, black, red)
            dst[k, pl.ds(2 * r + 1, n, stride=2), :] = jnp.where(m, red, black)


def correct(lv, s, src, start):
    for k in range(NL):
        for r, n in lv.chunks:
            x = src[k, pl.ds(start + r - 8, n), :]
            rows = pl.ds(r, n)
            for t in range(len(s["u"])):
                if lv.index > 0:
                    add = wide(x, 96 if lv.index == 1 else 64)
                else:
                    j = lanes(n)
                    add = take(x, (j >> 1) + 64 * t)
                for c in (0, 1):
                    s["u"][t][c, k, rows, :] = s["u"][t][c, k, rows, :] + add


def choose(label, entries):
    b0, b1, b2 = (label & 1) == 1, (label & 2) == 2, (label & 4) == 4
    low = [jnp.where(b0, entries[i + 1], entries[i]) for i in (0, 2, 4, 6)]
    return jnp.where(b2, jnp.where(b1, low[3], low[2]), jnp.where(b1, low[1], low[0]))


def clear_margins(lv, s):
    for t in range(len(s["u"])):
        for r in (0, 8 + lv.rows):
            zero = jnp.zeros((8, 128), F32)
            for c in (0, 1):
                for k in range(NL):
                    s["u"][t][c, k, pl.ds(r, 8), :] = zero
                    s["co"][t][c, 0, k, pl.ds(r, 8), :] = zero


def clear(lv, s):
    for k in range(NL):
        for r, n in lv.chunks:
            for c in (0, 1):
                s["u"][0][c, k, pl.ds(r, n), :] = jnp.zeros((n, 128), F32)


def coarse_solve(lv, s, r_ref, e_ref):
    u, cf, dg, iv = s["u"][0], s["cf"][0], s["dg"][0], s["iv"][0]
    cells = [(c, k, r, n) for c in (0, 1) for k in range(NL) for r, n in lv.chunks]

    def total(parts):
        while len(parts) > 1:
            parts = [a + b for a, b in zip(parts[::2], parts[1::2])] + ([parts[-1]] if len(parts) % 2 else [])
        return jnp.sum(jnp.sum(parts[0], axis=0, keepdims=True), axis=1, keepdims=True)

    parts = []
    for c, k, r, n in cells:
        rows = pl.ds(r, n)
        z = cf[c, 6, k, rows, :]
        f = dg[c, k, rows, :] * z
        u[c, k, rows, :] = z
        r_ref[c, k, rows, :] = f
        e_ref[c, k, rows, :] = jnp.zeros_like(f)
        parts.append(f * z)

    def step(i, inner):
        images, parts = [], []
        for c, k, r, n in cells:
            rows = pl.ds(r, n)
            search = u[c, k, rows, :]
            image = dg[c, k, rows, :] * (search - candidate(lv, s, 0, c, k, r, n))
            images.append(image)
            parts.append(search * image)
        alpha = inner / total(parts)
        parts = []
        for (c, k, r, n), image in zip(cells, images):
            rows = pl.ds(r, n)
            e_ref[c, k, rows, :] = e_ref[c, k, rows, :] + alpha * u[c, k, rows, :]
            left = r_ref[c, k, rows, :] - alpha * image
            r_ref[c, k, rows, :] = left
            parts.append(left * (left * iv[c, k, rows, :]))
        after = total(parts)
        beta = after / inner
        for c, k, r, n in cells:
            rows = pl.ds(r, n)
            u[c, k, rows, :] = r_ref[c, k, rows, :] * iv[c, k, rows, :] + beta * u[c, k, rows, :]
        return after

    lax.fori_loop(0, ITERS, step, total(parts))
    for c, k, r, n in cells:
        rows = pl.ds(r, n)
        u[c, k, rows, :] = e_ref[c, k, rows, :]


def halve(src, dst, arrays, rows):
    step = min(rows, 32)

    def one(a, _):
        for r in range(0, rows, step):
            even = src[a, pl.ds(2 * r, step, stride=2), :]
            other = src[a, pl.ds(2 * r + 1, step, stride=2), :]
            dst[a, pl.ds(r, step), :] = 0.25 * thin(even + other)
        return 0

    lax.fori_loop(0, arrays, one, 0)


def kernel(nx, ny, levels, heat_field, substance, category, planar, vertical, mass, wattage, out, *scratch):
    gx, gy = lax.axis_index("gx"), lax.axis_index("gy")
    place = (gx, gy, nx, ny)
    it = iter(scratch)
    st = []
    for lv in levels:
        tiles = 2 if lv.index == 0 else 1
        st.append({name: [next(it) for _ in range(tiles)] for name in ("u", "cf", "dg", "iv", "co")})
    ui, uh, cu0, cu1, cu2, cu3, cu4, cu5 = (next(it) for _ in range(8))
    f1, f3, f5, c1, c3, c5, sr, sp, cr, ce = (next(it) for _ in range(10))
    m0, k0, r0, q0 = (next(it) for _ in range(4))
    mc1, kc1, rc1, qc1, nc1 = (next(it) for _ in range(5))
    mf1, kf1, rf1, qf1, nf1 = (next(it) for _ in range(5))
    rr_c1, rr_f1 = next(it), next(it)
    b3c, g3c, b3f, g3f = (next(it) for _ in range(4))
    a5c, h5c, d5c, l5c = (next(it) for _ in range(4))
    a5f, h5f, d5f, l5f = (next(it) for _ in range(4))
    s0, s1c, s1f, s3c, s3f, s5c, s5f, s6c, s6f = (next(it) for _ in range(9))

    def exists(dx, dy):
        return (gx + dx >= 0) & (gx + dx < nx) & (gy + dy >= 0) & (gy + dy < ny)

    barrier = pltpu.get_barrier_semaphore()

    def greet_near(q, _):
        dx, dy = q // 5 - 2, lax.rem(q, 5) - 2

        @pl.when(exists(dx, dy) & (dx != 0) & (dy != 0))
        def _():
            pl.semaphore_signal(barrier, inc=1, device_id={"gx": gx + dx, "gy": gy + dy}, device_id_type=MESH)

        return 0

    lax.fori_loop(0, 25, greet_near, 0)

    def greet_gx(d, _):
        @pl.when(d != gx)
        def _():
            pl.semaphore_signal(barrier, inc=1, device_id={"gx": d}, device_id_type=MESH)

        return 0

    def greet_gy(d, _):
        @pl.when(d != gy)
        def _():
            pl.semaphore_signal(barrier, inc=1, device_id={"gy": d}, device_id_type=MESH)

        return 0

    lax.fori_loop(0, nx, greet_gx, 0)
    lax.fori_loop(0, ny, greet_gy, 0)

    def reach(at, size):
        return jnp.minimum(at, 2) + jnp.minimum(size - 1 - at, 2)

    for k in range(NL):
        for r in range(0, 128, 32):
            ui[k, pl.ds(8 + r, 32), :] = heat_field[k, pl.ds(r, 32), :]
            ui[NL + k, pl.ds(8 + r, 32), :] = substance[k, pl.ds(r, 32), :].astype(F32)
    for i in range(8):
        row = jnp.zeros((8, 128), F32)
        for jj in range(8):
            row = jnp.where((lanes(8) >> 4) == jj, wattage[category[i, jj]], row)
        ui[12, pl.ds(8 + 16 * i, 8), :] = row
        ui[12, pl.ds(16 + 16 * i, 8), :] = row

    def columns0(a, _):
        first, last = jnp.zeros((8, 128), F32), jnp.zeros((8, 128), F32)
        slot = lanes(8) >> 3
        for g in range(16):
            z = roll(ui[a, pl.ds(8 + 8 * g, 8), :], 8 * g)
            first = jnp.where(slot == g, z, first)
            last = jnp.where(slot == (g + 15) % 16, z, last)
        m0[0, a] = first
        m0[1, a] = last
        return 0

    lax.fori_loop(0, 13, columns0, 0)
    slot8 = lanes(8) >> 3
    for i, r in ((0, 8), (1, 128)):
        first, last = jnp.zeros((8, 128), F32), jnp.zeros((8, 128), F32)
        for a in range(13):
            z = roll(ui[a, pl.ds(r, 8), :], 8 * a)
            first = jnp.where(slot8 == a, z, first)
            last = jnp.where(slot8 == (a + 15) % 16, z, last)
        k0[2 * i] = first
        k0[2 * i + 1] = last

    pl.semaphore_wait(barrier, (nx - 1) + (ny - 1) + reach(gx, nx) * reach(gy, ny))

    SIDES = [(-1, 0), (1, 0), (0, -1), (0, 1), (-1, -1), (-1, 1), (1, -1), (1, 1)]

    def side_copy(i, src, dst, sems):
        dx, dy = SIDES[i]
        opposite = SIDES.index((-dx, -dy))
        return pltpu.make_async_remote_copy(
            src_ref=src, dst_ref=dst, send_sem=sems.at[0, i], recv_sem=sems.at[1, opposite],
            device_id={"gx": gx + dx, "gy": gy + dy}, device_id_type=MESH,
        )

    def sides(refs, sems, action):
        for i, (dx, dy) in enumerate(SIDES):
            @pl.when(exists(dx, dy))
            def _(i=i):
                copy = side_copy(i, refs[i][0], refs[i][1], sems)
                if action == "start":
                    copy.start()
                elif action == "sent":
                    copy.wait_send()

    def arrive(refs, sems):
        for i, (dx, dy) in enumerate(SIDES):
            opposite = SIDES.index((-dx, -dy))

            @pl.when(exists(dx, dy))
            def _(opposite=opposite):
                side_copy(opposite, refs[opposite][0], refs[opposite][1], sems).wait_recv()

    def absent(fills):
        for (dx, dy), ref in zip(SIDES, fills):
            @pl.when(jnp.logical_not(exists(dx, dy)))
            def _(ref=ref):
                ref[...] = jnp.zeros(ref.shape, F32)

    top, bottom = pl.ds(0, 8), pl.ds(136, 8)
    ex0 = [
        (ui.at[:, pl.ds(8, 8), :], ui.at[:, bottom, :]),
        (ui.at[:, pl.ds(128, 8), :], ui.at[:, top, :]),
        (m0.at[0], r0.at[1]),
        (m0.at[1], r0.at[0]),
        (k0.at[0], q0.at[3]),
        (k0.at[1], q0.at[2]),
        (k0.at[2], q0.at[1]),
        (k0.at[3], q0.at[0]),
    ]
    sides(ex0, s0, "start")
    absent([ui.at[:, top, :], ui.at[:, bottom, :], r0.at[0], r0.at[1], q0.at[0], q0.at[1], q0.at[2], q0.at[3]])

    tables = [[ref[i] for i in range(8)] for ref in (planar, vertical, mass)]

    def own(k, _):
        for r in range(0, 128, 16):
            label = substance[k, pl.ds(r, 16), :]
            for m in range(3):
                cu0[m * NL + k, pl.ds(r, 16), :] = choose(label, tables[m])
        return 0

    lax.fori_loop(0, NL, own, 0)
    cu4[...] = jnp.zeros(cu4.shape, F32)
    halve(cu0, cu1, 18, 64)
    halve(cu1, cu2, 18, 32)
    halve(cu2, cu3, 18, 16)
    halve(cu3, cu4, 18, 8)
    halve(cu4, cu5, 18, 8)

    def pack1(src, arrays, m, k, rws):
        slot = lanes(8) >> 5

        def one(a, _):
            for v in range(2):
                first, last = jnp.zeros((8, 128), F32), jnp.zeros((8, 128), F32)
                for q in range(4):
                    z = roll(src[a, pl.ds(32 * v + 8 * q, 8), :], 32 * q)
                    first = jnp.where(slot == q, z, first)
                    last = jnp.where(slot == (q + 1) % 4, z, last)
                m[0, a, pl.ds(8 * v, 8), :] = first
                m[1, a, pl.ds(8 * v, 8), :] = last
                k[2 * v, a] = first
                k[2 * v + 1, a] = last
                x = src[a, pl.ds(32 * v, 16), :]
                y = src[a, pl.ds(32 * v + 16, 16), :]
                rws[v, a] = jnp.where(lanes(16) < 64, x, roll(y, 64))
            return 0

        lax.fori_loop(0, arrays, one, 0)

    def exchange1(m, k, rws, r, q, n):
        return [
            (rws.at[0], n.at[1]), (rws.at[1], n.at[0]),
            (m.at[0], r.at[1]), (m.at[1], r.at[0]),
            (k.at[0], q.at[3]), (k.at[1], q.at[2]), (k.at[2], q.at[1]), (k.at[3], q.at[0]),
        ]

    def absent1(r, q, n):
        absent([n.at[0], n.at[1], r.at[0], r.at[1], q.at[0], q.at[1], q.at[2], q.at[3]])

    def unpack1(src, dst, arrays, r, q, n):
        slot, j8 = lanes(8) >> 5, lanes(8)

        def one(a, _):
            for v in range(2):
                own_rows, over = n[v, a], roll(n[v, a], 64)
                for g in range(4):
                    z = roll(jnp.where(slot == g, q[2 * v + 1, a], q[2 * v, a]), 64 - 32 * g)
                    x = (own_rows if g < 2 else over)[8 * (g % 2) : 8 * (g % 2) + 8]
                    dst[a, pl.ds(96 * v + 8 * g, 8), :] = jnp.where(j8 < 64, x, z)
                    y = roll(jnp.where(slot == g, r[1, a, pl.ds(8 * v, 8), :], r[0, a, pl.ds(8 * v, 8), :]), 64 - 32 * g)
                    x = src[a, pl.ds(32 * v + 8 * g, 8), :]
                    dst[a, pl.ds(32 + 32 * v + 8 * g, 8), :] = jnp.where(j8 < 64, x, y)
            return 0

        lax.fori_loop(0, arrays, one, 0)

    pack1(cu1, 18, mc1, kc1, rr_c1)
    exc1 = exchange1(mc1, kc1, rr_c1, rc1, qc1, nc1)
    sides(exc1, s1c, "start")
    absent1(rc1, qc1, nc1)

    def pack3(src, sets, dst):
        for m in range(sets):
            total = src[m * NL, pl.ds(0, 16), :]
            for k in range(1, NL):
                z = roll(src[m * NL + k, pl.ds(0, 16), :], 16 * k)
                total = jnp.where((lanes(16) >> 4) == k, z, total)
            dst[m] = total

    def near(action, src, dst, sems):
        def one(q, _):
            dx, dy = q // 5 - 2, lax.rem(q, 5) - 2

            @pl.when(exists(dx, dy) & (q != 12))
            def _():
                there = 24 - q
                if action == "arrive":
                    pltpu.make_async_remote_copy(
                        src_ref=src, dst_ref=dst.at[q], send_sem=sems.at[0, there], recv_sem=sems.at[1, q],
                        device_id={"gx": gx + dx, "gy": gy + dy}, device_id_type=MESH,
                    ).wait_recv()
                else:
                    copy = pltpu.make_async_remote_copy(
                        src_ref=src, dst_ref=dst.at[there], send_sem=sems.at[0, q], recv_sem=sems.at[1, there],
                        device_id={"gx": gx + dx, "gy": gy + dy}, device_id_type=MESH,
                    )
                    if action == "start":
                        copy.start()
                    else:
                        copy.wait_send()

            if action == "start":
                @pl.when(jnp.logical_not(exists(dx, dy)))
                def _():
                    dst[q] = jnp.zeros(dst.shape[1:], F32)

            return 0

        lax.fori_loop(0, 25, one, 0)

    def unpack3(src, got, sets, dst):
        j = lanes(16)
        slot = j >> 4
        for m in range(sets):
            def rows(x, _, m=m):
                for k in range(NL):
                    total = jnp.zeros((16, 128), F32)
                    for dy in range(-2, 3):
                        z = roll(got[x * 5 + dy + 2, m], 16 * dy - 16 * k)
                        total = jnp.where(slot == dy % 8, z, total)
                    dst[m * NL + k, pl.ds(pl.multiple_of(16 * x, 16), 16), :] = total
                return 0

            lax.fori_loop(0, 5, rows, 0)

    pack3(cu3, 3, b3c)
    near("start", b3c, g3c, s3c)
    g3c[12] = b3c[...]

    def pack5(src, arrays, dst):
        total = src[0, pl.ds(0, 8), :]
        for a in range(1, arrays):
            total = jnp.where((lanes(8) >> 2) == a, roll(src[a, pl.ds(0, 8), :], 4 * a), total)
        dst[...] = total

    def line(action, axis, me, size, src, dst, sems):
        def one(d, _):
            @pl.when(d != me)
            def _():
                if action == "arrive":
                    pltpu.make_async_remote_copy(
                        src_ref=src, dst_ref=dst.at[d], send_sem=sems.at[0, d], recv_sem=sems.at[1, d],
                        device_id={axis: d}, device_id_type=MESH,
                    ).wait_recv()
                else:
                    copy = pltpu.make_async_remote_copy(
                        src_ref=src, dst_ref=dst.at[me], send_sem=sems.at[0, d], recv_sem=sems.at[1, me],
                        device_id={axis: d}, device_id_type=MESH,
                    )
                    if action == "start":
                        copy.start()
                    else:
                        copy.wait_send()

            return 0

        lax.fori_loop(0, size, one, 0)

    def strip5(got, arrays, dst):
        j8 = lanes(8)
        low = lax.broadcasted_iota(jnp.int32, (8, 128), 0) < 4
        strips = []
        for a in range(arrays):
            total = jnp.zeros((8, 128), F32)
            for d in range(ny):
                total = jnp.where((j8 >> 2) == d, roll(got[d], 4 * d - 4 * a), total)
            strips.append(total)
        for t in range((arrays + 3) // 4):
            four = [strips[a] if a < arrays else jnp.zeros((8, 128), F32) for a in range(4 * t, 4 * t + 4)]
            x = jnp.where(j8 < 64, four[0], roll(four[1], 64))
            y = jnp.where(j8 < 64, four[2], roll(four[3], 64))
            dst[pl.ds(8 * t, 8), :] = jnp.where(low, x, pltpu.roll(y, 4, 0))

    def whole5(got, arrays, dst):
        j8 = lanes(8)
        low = lax.broadcasted_iota(jnp.int32, (8, 128), 0) < 4
        for a in range(arrays):
            t, up, right = a // 4, (a // 2) % 2, a % 2
            for h in range(nx // 2):
                x, y = got[2 * h, pl.ds(8 * t, 8), :], got[2 * h + 1, pl.ds(8 * t, 8), :]
                if up == 0:
                    y = pltpu.roll(y, 4, 0)
                else:
                    x = pltpu.roll(x, 4, 0)
                z = jnp.where(low, x, y)
                dst[a, pl.ds(8 * h, 8), :] = jnp.where(j8 < 64, roll(z, 64 * right), 0.0)

    pack5(cu5, 18, a5c)
    line("start", "gy", gy, ny, a5c, h5c, s5c)
    h5c[gy] = a5c[...]

    for lv, s in zip(levels, st):
        clear_margins(lv, s)
    for lv, s in list(zip(levels, st))[1:6]:
        clear(lv, s)
    for ref in (sr, sp):
        ref[...] = jnp.zeros(ref.shape, F32)

    arrive(ex0, s0)

    def beside0(a, _):
        slot = lanes(8) >> 3
        for g in range(16):
            uh[a, pl.ds(8 + 8 * g, 8), :] = roll(jnp.where(slot == g, r0[1, a], r0[0, a]), -8 * g)
        return 0

    lax.fori_loop(0, 13, beside0, 0)
    for i, r in ((0, 0), (1, 136)):
        for a in range(13):
            uh[a, pl.ds(r, 8), :] = roll(jnp.where(slot8 == a, q0[2 * i + 1], q0[2 * i]), -8 * a)

    lv, s = levels[0], st[0]
    for t, src in enumerate((ui, uh)):
        for r, n in lv.chunks:
            ok = inside(lv, t, r, n, *place)
            rows = pl.ds(r, n)
            for k in range(NL):
                label = pairs(src, NL + k, 0, lv, r, n)
                value = pairs(src, k, 0, lv, r, n)
                for c in (0, 1):
                    m = odd(n, k, c)
                    kind = jnp.where(m, label[1], label[0]).astype(jnp.int32)
                    s["u"][t][c, k, rows, :] = jnp.where(m, value[1], value[0])
                    s["co"][t][c, 0, k, rows, :] = jnp.where(ok, choose(kind, tables[0]), 0.0)
                    s["co"][t][c, 1, k, rows, :] = choose(kind, tables[1])
                    s["co"][t][c, 2, k, rows, :] = choose(kind, tables[2])
    weigh(lv, s, place)
    for t, src in enumerate((ui, uh)):
        for r, n in lv.chunks:
            rows = pl.ds(r, n)
            heat = pairs(src, 12, 0, lv, r, n)
            for k in range(NL):
                for c in (0, 1):
                    f = s["co"][t][c, 2, k, rows, :] * s["u"][t][c, k, rows, :]
                    if k == 0:
                        f = f + jnp.where(odd(n, k, c), heat[1], heat[0])
                    s["cf"][t][c, 6, k, rows, :] = s["iv"][t][c, k, rows, :] * f
    smooth(lv, s)
    restrict_rhs(lv, s, sr)
    for k in range(NL):
        for r in range(0, 64, 32):
            f5[k, pl.ds(r, 32), :] = sr[k, pl.ds(lv.base + r, 32), :]
    pack1(f5, 6, mf1, kf1, rr_f1)
    exf1 = exchange1(mf1, kf1, rr_f1, rf1, qf1, nf1)
    sides(exf1, s1f, "start")
    absent1(rf1, qf1, nf1)

    line("arrive", "gy", gy, ny, a5c, h5c, s5c)
    strip5(h5c, 18, d5c)
    arrive(exc1, s1c)
    unpack1(cu1, c1, 18, rc1, qc1, nc1)
    line("start", "gx", gx, nx, d5c, l5c, s6c)
    l5c[gx] = d5c[...]
    pack_coefficients(levels[1], st[1], c1, 0)
    weigh(levels[1], st[1], place)
    c1[...] = jnp.zeros(c1.shape, F32)
    restrict_coefficients(levels[1], st[1], c1)
    pack_coefficients(levels[2], st[2], c1, levels[1].base + 2 * (8 - levels[2].base))
    weigh(levels[2], st[2], place)

    arrive(exf1, s1f)
    unpack1(f5, f1, 6, rf1, qf1, nf1)
    pack_rhs(levels[1], st[1], f1, 0)
    smooth(levels[1], st[1])
    restrict_rhs(levels[1], st[1], sr)
    pack_rhs(levels[2], st[2], sr, levels[1].base + 2 * (8 - levels[2].base))
    smooth(levels[2], st[2])
    restrict_rhs(levels[2], st[2], sr)
    for k in range(NL):
        f3[k, pl.ds(0, 16), :] = sr[k, pl.ds(levels[2].base, 16), :]
    pack3(f3, 1, b3f)
    near("arrive", b3c, g3c, s3c)
    near("start", b3f, g3f, s3f)
    g3f[12] = b3f[...]
    unpack3(b3c, g3c, 3, c3)
    pack_coefficients(levels[3], st[3], c3, 0)
    weigh(levels[3], st[3], place)
    c1[...] = jnp.zeros(c1.shape, F32)
    restrict_coefficients(levels[3], st[3], c1)
    pack_coefficients(levels[4], st[4], c1, levels[3].base + 2 * (8 - levels[4].base))
    weigh(levels[4], st[4], place)
    sr[...] = jnp.zeros(sr.shape, F32)

    near("arrive", b3f, g3f, s3f)
    unpack3(b3f, g3f, 1, f3)
    pack_rhs(levels[3], st[3], f3, 0)
    smooth(levels[3], st[3])
    restrict_rhs(levels[3], st[3], sr)
    pack_rhs(levels[4], st[4], sr, levels[3].base + 2 * (8 - levels[4].base))
    smooth(levels[4], st[4])
    restrict_rhs(levels[4], st[4], sr)
    for k in range(NL):
        cu5[k, pl.ds(0, 8), :] = sr[k, pl.ds(levels[4].base, 8), :]
    pack5(cu5, 6, a5f)
    line("arrive", "gx", gx, nx, d5c, l5c, s6c)
    line("start", "gy", gy, ny, a5f, h5f, s5f)
    h5f[gy] = a5f[...]

    whole5(l5c, 18, c5)
    pack_coefficients(levels[5], st[5], c5, 0)
    weigh(levels[5], st[5], place)
    line("arrive", "gy", gy, ny, a5f, h5f, s5f)
    strip5(h5f, 6, d5f)
    c1[...] = jnp.zeros(c1.shape, F32)
    line("start", "gx", gx, nx, d5f, l5f, s6f)
    l5f[gx] = d5f[...]
    restrict_coefficients(levels[5], st[5], c1)
    pack_coefficients(levels[6], st[6], c1, 8)
    weigh(levels[6], st[6], place)
    sr[...] = jnp.zeros(sr.shape, F32)
    line("arrive", "gx", gx, nx, d5f, l5f, s6f)
    whole5(l5f, 6, f5)
    pack_rhs(levels[5], st[5], f5, 0)
    smooth(levels[5], st[5])
    restrict_rhs(levels[5], st[5], sr)
    pack_rhs(levels[6], st[6], sr, 8)
    coarse_solve(levels[6], st[6], cr, ce)

    sp[...] = jnp.zeros(sp.shape, F32)
    spread(levels[6], st[6], sp)
    correct(levels[5], st[5], sp, 2 * levels[6].base + 8 - levels[5].base)
    smooth(levels[5], st[5])
    sp[...] = jnp.zeros(sp.shape, F32)
    spread(levels[5], st[5], sp)
    lv, s = levels[4], st[4]
    first = 2 * levels[5].base + 8 - lv.base + 4 * gx
    for k in range(NL):
        x = sp[k, pl.ds(first, lv.rows), :]
        add = wide(pltpu.roll(x, lax.rem(128 - 4 * gy, 128), 1))
        for c in (0, 1):
            rows = pl.ds(8, lv.rows)
            s["u"][0][c, k, rows, :] = s["u"][0][c, k, rows, :] + add
    smooth(lv, s)
    for i in (3, 2, 1, 0):
        sp[...] = jnp.zeros(sp.shape, F32)
        spread(levels[i + 1], st[i + 1], sp)
        correct(levels[i], st[i], sp, 2 * levels[i + 1].base + 8 - levels[i].base)
        smooth(levels[i], st[i])
    u = st[0]["u"][0]
    for k in range(NL):
        for r in range(0, 64, 32):
            red, black = u[0, k, pl.ds(levels[0].base + r, 32), :], u[1, k, pl.ds(levels[0].base + r, 32), :]
            m = odd(32, k, 0)
            out[k, pl.ds(2 * r, 32, stride=2), :] = jnp.where(m, black, red)
            out[k, pl.ds(2 * r + 1, 32, stride=2), :] = jnp.where(m, red, black)

    sides(ex0, s0, "sent")
    sides(exc1, s1c, "sent")
    sides(exf1, s1f, "sent")
    near("sent", b3c, g3c, s3c)
    near("sent", b3f, g3f, s3f)
    line("sent", "gy", gy, ny, a5c, h5c, s5c)
    line("sent", "gy", gy, ny, a5f, h5f, s5f)
    line("sent", "gx", gx, nx, d5c, l5c, s6c)
    line("sent", "gx", gx, nx, d5f, l5f, s6f)


def solution(mesh):
    nx, ny = mesh.shape["gx"], mesh.shape["gy"]
    levels = [
        Level(0, 128, 12, 72, 8),
        Level(1, 64, 24, 64, 32),
        Level(2, 32, 16, 32, 16),
        Level(3, 16, 24, 40, 32),
        Level(4, 8, 16, 24, 16),
        Level(5, 4, 8, 2 * nx, 0, True),
        Level(6, 2, 8, max(8, nx), 0, True),
    ]

    def buffer(*shape):
        return pltpu.VMEM(shape, F32)

    scratch = []
    for lv in levels:
        tiles = 2 if lv.index == 0 else 1
        n = lv.total
        for shape in ((2, 6, n, 128), (2, 7, 6, n, 128), (2, 6, n, 128), (2, 6, n, 128), (2, 3, 6, n, 128)):
            scratch += [buffer(*shape)] * tiles
    scratch += [buffer(13, 144, 128)] * 2
    scratch += [buffer(18, n, 128) for n in (128, 64, 32, 16, 16, 8)]
    scratch += [buffer(6, 128, 128), buffer(6, 80, 128), buffer(6, max(64, 4 * nx), 128)]
    scratch += [buffer(18, 128, 128), buffer(18, 80, 128), buffer(18, 4 * nx, 128)]
    scratch += [buffer(6, 96, 128), buffer(6, 160, 128)]
    n = levels[6].total
    scratch += [buffer(2, 6, n, 128)] * 2
    scratch += [buffer(2, 13, 8, 128), buffer(4, 8, 128), buffer(2, 13, 8, 128), buffer(4, 8, 128)]
    for a in (18, 6):
        scratch += [buffer(2, a, 16, 128), buffer(4, a, 8, 128), buffer(2, a, 16, 128), buffer(4, a, 8, 128), buffer(2, a, 16, 128)]
    scratch += [buffer(2, 18, 16, 128), buffer(2, 6, 16, 128)]
    scratch += [buffer(3, 16, 128), buffer(25, 3, 16, 128), buffer(1, 16, 128), buffer(25, 1, 16, 128)]
    for rows in (40, 16):
        scratch += [buffer(8, 128), buffer(ny, 8, 128), buffer(rows, 128), buffer(nx, rows, 128)]
    scratch += [pltpu.SemaphoreType.DMA((2, 8))] * 3 + [pltpu.SemaphoreType.DMA((2, 25))] * 2
    scratch += [pltpu.SemaphoreType.DMA((2, ny))] * 2 + [pltpu.SemaphoreType.DMA((2, nx))] * 2

    def on_device(*args):
        vmem, smem = pl.BlockSpec(memory_space=pltpu.VMEM), pl.BlockSpec(memory_space=pltpu.SMEM)

        def body(*refs):
            kernel(nx, ny, levels, *refs)

        return pl.pallas_call(
            body,
            out_shape=jax.ShapeDtypeStruct((6, 128, 128), F32),
            in_specs=[vmem, vmem] + [smem] * 5,
            out_specs=vmem,
            scratch_shapes=scratch,
            compiler_params=pltpu.CompilerParams(
                collective_id=0, has_side_effects=True, vmem_limit_bytes=60 * 2**20
            ),
            name="vcycle",
        )(*args)

    placed = (P(None, "gx", "gy"), P(None, "gx", "gy"), P("gx", "gy"), P(), P(), P(), P())
    return jax.shard_map(on_device, mesh=mesh, in_specs=placed, out_specs=P(None, "gx", "gy"), check_vma=False)
```

```python
import jax
import jax.numpy as jnp
from jax import lax
from jax.experimental import pallas as pl
from jax.experimental.pallas import tpu as pltpu
from jax.sharding import PartitionSpec as P

MESH = pl.DeviceIdType.MESH
NL = 6
TILE = 16
ITERS = 12
F32 = jnp.float32


class Level:
    def __init__(self, index, block, base, rows, half, whole=False):
        self.index, self.block, self.base, self.rows, self.half, self.whole = index, block, base, rows, half, whole
        self.total = rows + 16
        self.scale = 0.25**index
        step = 24 if rows % 24 == 0 else 16 if rows % 16 == 0 else 8
        self.chunks = [(r, min(step, 8 + rows - r)) for r in range(8, 8 + rows, step)]


def lanes(n):
    return lax.broadcasted_iota(jnp.int32, (n, 128), 1)


def odd(n, k, c):
    bit = lanes(n) & 1
    return bit == 1 if (k + c) % 2 == 0 else bit == 0


def roll(x, shift):
    shift %= 128
    return x if shift == 0 else pltpu.roll(x, shift, 1)


def take(x, index):
    return jnp.take_along_axis(x, index, axis=1, mode="promise_in_bounds")


def thin(ref, spots):
    for a, r, n in spots:
        x = ref[a, pl.ds(r, n), :]
        ref[a, pl.ds(r, n), :] = 0.25 * (x + roll(x, 127))
    for a, r, n in spots:
        x = ref[a, pl.ds(r, n), :]
        ref[a, pl.ds(r, n), :] = take(x, (2 * lanes(n)) & 127)


def wide(x, split=64):
    j = lanes(x.shape[0])
    return take(x, jnp.where(j < split, j >> 1, 64 + (j >> 1)))


def around(refs, t, o, k, r, n, c, pick=()):
    ref = refs[t]
    here = ref[(o, *pick, k, pl.ds(r, n), slice(None))]
    before = ref[(o, *pick, k, pl.ds(r - 1, n), slice(None))]
    after = ref[(o, *pick, k, pl.ds(r + 1, n), slice(None))]
    far = jnp.where(odd(n, k, c), after, before)
    left, right = roll(here, 1), roll(here, 127)
    if len(refs) == 2:
        j = lanes(n)
        beside = refs[1 - t][(o, *pick, k, pl.ds(r, n), slice(None))]
        left = jnp.where(j == 0, roll(beside, 1), left)
        right = jnp.where(j == 127, roll(beside, 127), right)
    return here, far, left, right


def candidate(lv, s, t, c, k, r, n):
    o = 1 - c
    cf = s["cf"][t]
    here, far, left, right = around(s["u"], t, o, k, r, n, c)
    rows = pl.ds(r, n)
    a = cf[c, 0, k, rows, :] * here + cf[c, 1, k, rows, :] * far
    b = cf[c, 2, k, rows, :] * left + cf[c, 3, k, rows, :] * right
    if k > 0:
        a = a + cf[c, 4, k, rows, :] * s["u"][t][o, k - 1, rows, :]
    if k < NL - 1:
        b = b + cf[c, 5, k, rows, :] * s["u"][t][o, k + 1, rows, :]
    return a + b


def half_sweep(lv, s, c):
    for t in range(len(s["u"])):
        for k in range(NL):
            for r, n in lv.chunks:
                rows = pl.ds(r, n)
                s["u"][t][c, k, rows, :] = s["cf"][t][c, 6, k, rows, :] + candidate(lv, s, t, c, k, r, n)


def smooth(lv, s):
    def sweep(i, _):
        half_sweep(lv, s, 0)
        half_sweep(lv, s, 1)
        return 0

    lax.fori_loop(0, 2, sweep, 0)


def residual(lv, s, t, k, r, n):
    rows = pl.ds(r, n)
    parts = []
    for c in (0, 1):
        new = s["cf"][t][c, 6, k, rows, :] + candidate(lv, s, t, c, k, r, n)
        parts.append(s["dg"][t][c, k, rows, :] * (new - s["u"][t][c, k, rows, :]))
    return parts[0] + parts[1]


def inside(lv, t, r, n, gx, gy, nx, ny):
    row = lax.broadcasted_iota(jnp.int32, (n, 128), 0) + (r - lv.base)
    j = lanes(n)
    if lv.whole:
        return (row >= 0) & (row < lv.block * nx // 2) & (j < lv.block * ny)
    half = lv.half // 2
    if lv.index == 0:
        col = j if t == 0 else jnp.where(j < 64, j + 128, j - 128)
    elif lv.index == 1:
        col = jnp.where(j < 96, j, j - 128)
    else:
        col = jnp.where(j < 64, j, j - 128)
    ok = (row >= -half) & (row < lv.block // 2 + half) & (col >= -lv.half) & (col < lv.block + lv.half)
    row, col = row + gx * (lv.block // 2), col + gy * lv.block
    return ok & (row >= 0) & (row < lv.block * nx // 2) & (col >= 0) & (col < lv.block * ny)


def weigh(lv, s, place):
    h = 0.5 * lv.scale
    for t in range(len(s["u"])):
        co = s["co"]
        for r, n in lv.chunks:
            ok = inside(lv, t, r, n, *place)
            rows = pl.ds(r, n)
            for c in (0, 1):
                o = 1 - c
                for k in range(NL):
                    own = co[t][c, 0, k, rows, :]
                    ws = [h * (own + x) for x in around(co, t, o, k, r, n, c, (0,))]
                    diag = co[t][c, 2, k, rows, :] + ((ws[0] + ws[1]) + (ws[2] + ws[3]))
                    mine = co[t][c, 1, k, rows, :]
                    for other, there in ((k - 1, k > 0), (k + 1, k < NL - 1)):
                        if there:
                            face = 0.5 * (mine + co[t][o, 1, other, rows, :])
                            diag = diag + face
                            ws.append(face)
                        else:
                            ws.append(None)
                    inv = jnp.where(ok, 1.0 / diag, 0.0)
                    for i, w in enumerate(ws):
                        if w is not None:
                            s["cf"][t][c, i, k, rows, :] = w * inv
                    s["dg"][t][c, k, rows, :] = diag
                    s["iv"][t][c, k, rows, :] = inv


def pairs(ref, a, start, lv, r, n):
    first = start + 2 * (r - 8)
    even = ref[a, pl.ds(first, n, stride=2), :]
    other = ref[a, pl.ds(first + 1, n, stride=2), :]
    return even, other


def pack_coefficients(lv, s, src, start):
    for m in range(3):
        for k in range(NL):
            for r, n in lv.chunks:
                even, other = pairs(src, m * NL + k, start, lv, r, n)
                for c in (0, 1):
                    s["co"][0][c, m, k, pl.ds(r, n), :] = jnp.where(odd(n, k, c), other, even)


def pack_rhs(lv, s, src, start):
    for k in range(NL):
        for r, n in lv.chunks:
            even, other = pairs(src, k, start, lv, r, n)
            rows = pl.ds(r, n)
            for c in (0, 1):
                f = jnp.where(odd(n, k, c), other, even)
                s["cf"][0][c, 6, k, rows, :] = s["iv"][0][c, k, rows, :] * f


def restrict_rhs(lv, s, dst):
    for k in range(NL):
        for r, n in lv.chunks:
            dst[k, pl.ds(r, n), :] = residual(lv, s, 0, k, r, n)
    thin(dst, [(k, r, n) for k in range(NL) for r, n in lv.chunks])


def restrict_coefficients(lv, s, dst):
    for m in range(3):
        for k in range(NL):
            for r, n in lv.chunks:
                rows = pl.ds(r, n)
                dst[m * NL + k, rows, :] = s["co"][0][0, m, k, rows, :] + s["co"][0][1, m, k, rows, :]
    thin(dst, [(a, r, n) for a in range(3 * NL) for r, n in lv.chunks])


def spread(lv, s, dst):
    for k in range(NL):
        for r, n in lv.chunks:
            red, black = s["u"][0][0, k, pl.ds(r, n), :], s["u"][0][1, k, pl.ds(r, n), :]
            m = odd(n, k, 0)
            dst[k, pl.ds(2 * r, n, stride=2), :] = jnp.where(m, black, red)
            dst[k, pl.ds(2 * r + 1, n, stride=2), :] = jnp.where(m, red, black)


def correct(lv, s, src, start):
    for k in range(NL):
        for r, n in lv.chunks:
            x = src[k, pl.ds(start + r - 8, n), :]
            rows = pl.ds(r, n)
            for t in range(len(s["u"])):
                if lv.index > 0:
                    add = wide(x, 96 if lv.index == 1 else 64)
                else:
                    j = lanes(n)
                    add = take(x, (j >> 1) + 64 * t)
                for c in (0, 1):
                    s["u"][t][c, k, rows, :] = s["u"][t][c, k, rows, :] + add


def choose(label, entries):
    b0, b1, b2 = (label & 1) == 1, (label & 2) == 2, (label & 4) == 4
    low = [jnp.where(b0, entries[i + 1], entries[i]) for i in (0, 2, 4, 6)]
    return jnp.where(b2, jnp.where(b1, low[3], low[2]), jnp.where(b1, low[1], low[0]))


def clear_margins(lv, s):
    for t in range(len(s["u"])):
        for r in (0, 8 + lv.rows):
            zero = jnp.zeros((8, 128), F32)
            for c in (0, 1):
                for k in range(NL):
                    s["u"][t][c, k, pl.ds(r, 8), :] = zero
                    s["co"][t][c, 0, k, pl.ds(r, 8), :] = zero


def clear(lv, s):
    for k in range(NL):
        for r, n in lv.chunks:
            for c in (0, 1):
                s["u"][0][c, k, pl.ds(r, n), :] = jnp.zeros((n, 128), F32)


def coarse_solve(lv, s, r_ref, p_ref, q_ref, e_ref):
    u, cf, dg, iv = s["u"][0], s["cf"][0], s["dg"][0], s["iv"][0]
    cells = [(c, k, r, n) for c in (0, 1) for k in range(NL) for r, n in lv.chunks]

    def total(parts):
        while len(parts) > 1:
            parts = [a + b for a, b in zip(parts[::2], parts[1::2])] + ([parts[-1]] if len(parts) % 2 else [])
        return jnp.sum(jnp.sum(parts[0], axis=0, keepdims=True), axis=1, keepdims=True)

    def images():
        ws, rz, zw = [], [], []
        for c, k, r, n in cells:
            rows = pl.ds(r, n)
            z = u[c, k, rows, :]
            w = dg[c, k, rows, :] * (z - candidate(lv, s, 0, c, k, r, n))
            ws.append(w)
            rz.append(r_ref[c, k, rows, :] * z)
            zw.append(z * w)
        return ws, total(rz), total(zw)

    for c, k, r, n in cells:
        rows = pl.ds(r, n)
        z = cf[c, 6, k, rows, :]
        u[c, k, rows, :] = z
        r_ref[c, k, rows, :] = dg[c, k, rows, :] * z
    ws, rz, zw = images()
    for (c, k, r, n), w in zip(cells, ws):
        rows = pl.ds(r, n)
        p_ref[c, k, rows, :] = u[c, k, rows, :]
        q_ref[c, k, rows, :] = w
        e_ref[c, k, rows, :] = jnp.zeros_like(w)

    def step(i, carry):
        rz, alpha = carry
        for c, k, r, n in cells:
            rows = pl.ds(r, n)
            left = r_ref[c, k, rows, :] - alpha * q_ref[c, k, rows, :]
            r_ref[c, k, rows, :] = left
            u[c, k, rows, :] = left * iv[c, k, rows, :]
            e_ref[c, k, rows, :] = e_ref[c, k, rows, :] + alpha * p_ref[c, k, rows, :]
        ws, after, zw = images()
        beta = after / rz
        for (c, k, r, n), w in zip(cells, ws):
            rows = pl.ds(r, n)
            p_ref[c, k, rows, :] = u[c, k, rows, :] + beta * p_ref[c, k, rows, :]
            q_ref[c, k, rows, :] = w + beta * q_ref[c, k, rows, :]
        return after, after / (zw - beta * after / alpha)

    rz, alpha = lax.fori_loop(0, ITERS - 1, step, (rz, rz / zw))
    for c, k, r, n in cells:
        rows = pl.ds(r, n)
        u[c, k, rows, :] = e_ref[c, k, rows, :] + alpha * p_ref[c, k, rows, :]


def halve(src, dst, arrays, rows):
    step = min(rows, 32)
    spots = [(a, r, step) for a in range(arrays) for r in range(0, rows, step)]
    for a, r, n in spots:
        dst[a, pl.ds(r, n), :] = src[a, pl.ds(2 * r, n, stride=2), :] + src[a, pl.ds(2 * r + 1, n, stride=2), :]
    thin(dst, spots)


def kernel(nx, ny, levels, heat_field, substance, category, planar, vertical, mass, wattage, out, *scratch):
    gx, gy = lax.axis_index("gx"), lax.axis_index("gy")
    place = (gx, gy, nx, ny)
    half, core = nx // 2, lax.rem(gx, 2)
    at5 = core * half + gx // 2
    it = iter(scratch)
    st = []
    for lv in levels:
        tiles = 2 if lv.index == 0 else 1
        st.append({name: [next(it) for _ in range(tiles)] for name in ("u", "cf", "dg", "iv", "co")})
    ui, uh, cu0, cu1, cu2, cu3, cu4, cu5 = (next(it) for _ in range(8))
    f1, f3, f5, c1, c3, c5, sr, sp, cr, cp, cq, ce = (next(it) for _ in range(12))
    m0, k0, r0, q0 = (next(it) for _ in range(4))
    mc1, kc1, rc1, qc1, nc1 = (next(it) for _ in range(5))
    mf1, kf1, rf1, qf1, nf1 = (next(it) for _ in range(5))
    rr_c1, rr_f1 = next(it), next(it)
    b3c, g3c, b3f, g3f = (next(it) for _ in range(4))
    a5c, h5c, d5c, l5c = (next(it) for _ in range(4))
    a5f, h5f, d5f, l5f = (next(it) for _ in range(4))
    s0, s1c, s1f, s3c, s3f, s5c, s5f, s6c, s6f, s7c = (next(it) for _ in range(10))

    def exists(dx, dy):
        return (gx + dx >= 0) & (gx + dx < nx) & (gy + dy >= 0) & (gy + dy < ny)

    for q in range(25):
        if q != 12:
            g3c[q] = jnp.zeros(g3c.shape[1:], F32)
            g3f[q] = jnp.zeros(g3f.shape[1:], F32)
    barrier = pltpu.get_barrier_semaphore()

    def greet(**where):
        pl.semaphore_signal(barrier, inc=1, device_id=where, device_id_type=MESH)

    for dx in (-2, -1, 1, 2):
        for dy in (-2, -1, 1, 2):
            pl.when(exists(dx, dy))(lambda dx=dx, dy=dy: greet(gx=gx + dx, gy=gy + dy))
    for d in range(1, nx):
        greet(gx=lax.rem(gx + d, nx))
    for d in range(1, ny):
        greet(gy=lax.rem(gy + d, ny))

    def reach(at, size):
        return jnp.minimum(at, 2) + jnp.minimum(size - 1 - at, 2)

    for k in range(NL):
        for r in range(0, 128, 32):
            ui[k, pl.ds(8 + r, 32), :] = heat_field[k, pl.ds(r, 32), :]
            ui[NL + k, pl.ds(8 + r, 32), :] = substance[k, pl.ds(r, 32), :].astype(F32)
    for i in range(8):
        row = jnp.zeros((8, 128), F32)
        for jj in range(8):
            row = jnp.where((lanes(8) >> 4) == jj, wattage[category[i, jj]], row)
        ui[12, pl.ds(8 + 16 * i, 8), :] = row
        ui[12, pl.ds(16 + 16 * i, 8), :] = row

    for a in range(13):
        first, last = jnp.zeros((8, 128), F32), jnp.zeros((8, 128), F32)
        slot = lanes(8) >> 3
        for g in range(16):
            z = roll(ui[a, pl.ds(8 + 8 * g, 8), :], 8 * g)
            first = jnp.where(slot == g, z, first)
            last = jnp.where(slot == (g + 15) % 16, z, last)
        m0[0, a] = first
        m0[1, a] = last
    slot8 = lanes(8) >> 3
    for i, r in ((0, 8), (1, 128)):
        first, last = jnp.zeros((8, 128), F32), jnp.zeros((8, 128), F32)
        for a in range(13):
            z = roll(ui[a, pl.ds(r, 8), :], 8 * a)
            first = jnp.where(slot8 == a, z, first)
            last = jnp.where(slot8 == (a + 15) % 16, z, last)
        k0[2 * i] = first
        k0[2 * i + 1] = last

    tables = [[ref[i] for i in range(8)] for ref in (planar, vertical, mass)]

    def own(k, _):
        for r in range(0, 128, 16):
            label = substance[k, pl.ds(r, 16), :]
            for m in range(3):
                cu0[m * NL + k, pl.ds(r, 16), :] = choose(label, tables[m])
        return 0

    lax.fori_loop(0, NL, own, 0)
    cu4[...] = jnp.zeros(cu4.shape, F32)
    halve(cu0, cu1, 18, 64)

    pl.semaphore_wait(barrier, (nx - 1) + (ny - 1) + reach(gx, nx) * reach(gy, ny))

    SIDES = [(-1, 0), (1, 0), (0, -1), (0, 1), (-1, -1), (-1, 1), (1, -1), (1, 1)]

    def side_copy(i, src, dst, sems):
        dx, dy = SIDES[i]
        opposite = SIDES.index((-dx, -dy))
        return pltpu.make_async_remote_copy(
            src_ref=src, dst_ref=dst, send_sem=sems.at[0, i], recv_sem=sems.at[1, opposite],
            device_id={"gx": gx + dx, "gy": gy + dy}, device_id_type=MESH,
        )

    def sides(refs, sems, action):
        for i, (dx, dy) in enumerate(SIDES):
            @pl.when(exists(dx, dy))
            def _(i=i):
                copy = side_copy(i, refs[i][0], refs[i][1], sems)
                if action == "start":
                    copy.start()
                elif action == "sent":
                    copy.wait_send()

    def arrive(refs, sems):
        for i, (dx, dy) in enumerate(SIDES):
            opposite = SIDES.index((-dx, -dy))

            @pl.when(exists(dx, dy))
            def _(opposite=opposite):
                side_copy(opposite, refs[opposite][0], refs[opposite][1], sems).wait_recv()

    def absent(fills):
        for (dx, dy), ref in zip(SIDES, fills):
            @pl.when(jnp.logical_not(exists(dx, dy)))
            def _(ref=ref):
                ref[...] = jnp.zeros(ref.shape, F32)

    top, bottom = pl.ds(0, 8), pl.ds(136, 8)
    ex0 = [
        (ui.at[:, pl.ds(8, 8), :], ui.at[:, bottom, :]),
        (ui.at[:, pl.ds(128, 8), :], ui.at[:, top, :]),
        (m0.at[0], r0.at[1]),
        (m0.at[1], r0.at[0]),
        (k0.at[0], q0.at[3]),
        (k0.at[1], q0.at[2]),
        (k0.at[2], q0.at[1]),
        (k0.at[3], q0.at[0]),
    ]
    sides(ex0, s0, "start")
    absent([ui.at[:, top, :], ui.at[:, bottom, :], r0.at[0], r0.at[1], q0.at[0], q0.at[1], q0.at[2], q0.at[3]])

    def pack1(src, arrays, m, k, rws):
        slot = lanes(8) >> 5

        def one(i, _):
            for a, v in [(3 * i + e, v) for e in range(3) for v in range(2)]:
                first, last = jnp.zeros((8, 128), F32), jnp.zeros((8, 128), F32)
                for q in range(4):
                    z = roll(src[a, pl.ds(32 * v + 8 * q, 8), :], 32 * q)
                    first = jnp.where(slot == q, z, first)
                    last = jnp.where(slot == (q + 1) % 4, z, last)
                m[0, a, pl.ds(8 * v, 8), :] = first
                m[1, a, pl.ds(8 * v, 8), :] = last
                k[2 * v, a] = first
                k[2 * v + 1, a] = last
                x = src[a, pl.ds(32 * v, 16), :]
                y = src[a, pl.ds(32 * v + 16, 16), :]
                rws[v, a] = jnp.where(lanes(16) < 64, x, roll(y, 64))
            return 0

        lax.fori_loop(0, arrays // 3, one, 0)

    def exchange1(m, k, rws, r, q, n):
        return [
            (rws.at[0], n.at[1]), (rws.at[1], n.at[0]),
            (m.at[0], r.at[1]), (m.at[1], r.at[0]),
            (k.at[0], q.at[3]), (k.at[1], q.at[2]), (k.at[2], q.at[1]), (k.at[3], q.at[0]),
        ]

    def absent1(r, q, n):
        absent([n.at[0], n.at[1], r.at[0], r.at[1], q.at[0], q.at[1], q.at[2], q.at[3]])

    def unpack1(src, dst, arrays, r, q, n):
        slot, j8 = lanes(8) >> 5, lanes(8)

        def one(i, _):
            for a, v in [(3 * i + e, v) for e in range(3) for v in range(2)]:
                own_rows, over = n[v, a], roll(n[v, a], 64)
                for g in range(4):
                    z = roll(jnp.where(slot == g, q[2 * v + 1, a], q[2 * v, a]), 64 - 32 * g)
                    x = (own_rows if g < 2 else over)[8 * (g % 2) : 8 * (g % 2) + 8]
                    dst[a, pl.ds(96 * v + 8 * g, 8), :] = jnp.where(j8 < 64, x, z)
                    y = roll(jnp.where(slot == g, r[1, a, pl.ds(8 * v, 8), :], r[0, a, pl.ds(8 * v, 8), :]), 64 - 32 * g)
                    x = src[a, pl.ds(32 * v + 8 * g, 8), :]
                    dst[a, pl.ds(32 + 32 * v + 8 * g, 8), :] = jnp.where(j8 < 64, x, y)
            return 0

        lax.fori_loop(0, arrays // 3, one, 0)

    def pack3(src, sets, dst):
        for m in range(sets):
            total = src[m * NL, pl.ds(0, 16), :]
            for k in range(1, NL):
                z = roll(src[m * NL + k, pl.ds(0, 16), :], 16 * k)
                total = jnp.where((lanes(16) >> 4) == k, z, total)
            dst[m] = total

    def near(action, src, dst, sems):
        if action == "start":
            for q in [q for q in range(25) if q != 12]:
                dx, dy = q // 5 - 2, q % 5 - 2

                @pl.when(exists(dx, dy))
                def _(dx=dx, dy=dy, q=q):
                    pltpu.make_async_remote_copy(
                        src_ref=src, dst_ref=dst.at[24 - q], send_sem=sems.at[0], recv_sem=sems.at[1],
                        device_id={"gx": gx + dx, "gy": gy + dy}, device_id_type=MESH,
                    ).start()

            return
        for a in (2, 3, 4):
            for b in (2, 3, 4):
                @pl.when((reach(gx, nx) == a) & (reach(gy, ny) == b))
                def _(count=(a + 1) * (b + 1) - 1):
                    part = dst.at[pl.ds(0, count)]
                    pltpu.make_async_copy(part, part, sems.at[1 if action == "arrive" else 0]).wait()

    def unpack3(src, got, sets, dst):
        j = lanes(16)
        slot = j >> 4
        for m in range(sets):
            for x in range(5):
                for k in range(NL):
                    total = jnp.zeros((16, 128), F32)
                    for dy in range(-2, 3):
                        z = roll(got[x * 5 + dy + 2, m], 16 * dy - 16 * k)
                        total = jnp.where(slot == dy % 8, z, total)
                    dst[m * NL + k, pl.ds(16 * x, 16), :] = total

    def pack5(src, arrays, dst):
        total = src[0, pl.ds(0, 8), :]
        for a in range(1, arrays):
            total = jnp.where((lanes(8) >> 2) == a, roll(src[a, pl.ds(0, 8), :], 4 * a), total)
        dst[...] = total

    def line(action, axis, me, size, src, dst, sems):
        if action == "start":
            for d in range(1, size):
                pltpu.make_async_remote_copy(
                    src_ref=src, dst_ref=dst.at[me], send_sem=sems.at[0], recv_sem=sems.at[1],
                    device_id={axis: lax.rem(me + d, size)}, device_id_type=MESH,
                ).start()
            return
        part = dst.at[pl.ds(0, size - 1)]
        pltpu.make_async_copy(part, part, sems.at[1 if action == "arrive" else 0]).wait()

    def strip5(got, arrays, dst):
        j8 = lanes(8)
        low = lax.broadcasted_iota(jnp.int32, (8, 128), 0) < 4
        strips = []
        for a in range(arrays):
            total = jnp.zeros((8, 128), F32)
            for d in range(ny):
                total = jnp.where((j8 >> 2) == d, roll(got[d], 4 * d - 4 * a), total)
            strips.append(total)
        for t in range((arrays + 3) // 4):
            four = [strips[a] if a < arrays else jnp.zeros((8, 128), F32) for a in range(4 * t, 4 * t + 4)]
            x = jnp.where(j8 < 64, four[0], roll(four[1], 64))
            y = jnp.where(j8 < 64, four[2], roll(four[3], 64))
            dst[pl.ds(8 * t, 8), :] = jnp.where(low, x, pltpu.roll(y, 4, 0))

    def whole5(got, arrays, dst, order):
        j8 = lanes(8)
        low = lax.broadcasted_iota(jnp.int32, (8, 128), 0) < 4
        for a in range(arrays):
            t, up, right = a // 4, (a // 2) % 2, a % 2
            for h in range(nx // 2):
                x, y = got[order(2 * h), pl.ds(8 * t, 8), :], got[order(2 * h + 1), pl.ds(8 * t, 8), :]
                if up == 0:
                    y = pltpu.roll(y, 4, 0)
                else:
                    x = pltpu.roll(x, 4, 0)
                z = jnp.where(low, x, y)
                dst[a, pl.ds(8 * h, 8), :] = jnp.where(j8 < 64, roll(z, 64 * right), 0.0)

    exc1 = exchange1(mc1, kc1, rr_c1, rc1, qc1, nc1)
    pack1(cu1, 18, mc1, kc1, rr_c1)
    halve(cu1, cu2, 18, 32)
    sides(exc1, s1c, "start")
    halve(cu2, cu3, 18, 16)
    halve(cu3, cu4, 18, 8)
    halve(cu4, cu5, 18, 8)
    pack5(cu5, 18, a5c)
    pack3(cu3, 3, b3c)
    absent1(rc1, qc1, nc1)
    line("start", "gy", gy, ny, a5c, h5c, s5c)
    h5c[gy] = a5c[...]

    for lv, s in zip(levels, st):
        clear_margins(lv, s)
    for lv, s in list(zip(levels, st))[1:6]:
        clear(lv, s)
    for k in range(NL):
        for r in (8, 80, 88):
            sp[k, pl.ds(r, 8), :] = jnp.zeros((8, 128), F32)

    arrive(ex0, s0)

    for a in range(13):
        for g in range(16):
            uh[a, pl.ds(8 + 8 * g, 8), :] = roll(jnp.where(slot8 == g, r0[1, a], r0[0, a]), -8 * g)
    for i, r in ((0, 0), (1, 136)):
        for a in range(13):
            uh[a, pl.ds(r, 8), :] = roll(jnp.where(slot8 == a, q0[2 * i + 1], q0[2 * i]), -8 * a)

    lv, s = levels[0], st[0]
    for t, src in enumerate((ui, uh)):
        for r, n in lv.chunks:
            ok = inside(lv, t, r, n, *place)
            rows = pl.ds(r, n)
            for k in range(NL):
                label = pairs(src, NL + k, 0, lv, r, n)
                value = pairs(src, k, 0, lv, r, n)
                for c in (0, 1):
                    m = odd(n, k, c)
                    kind = jnp.where(m, label[1], label[0]).astype(jnp.int32)
                    s["u"][t][c, k, rows, :] = jnp.where(m, value[1], value[0])
                    s["co"][t][c, 0, k, rows, :] = jnp.where(ok, choose(kind, tables[0]), 0.0)
                    s["co"][t][c, 1, k, rows, :] = choose(kind, tables[1])
                    s["co"][t][c, 2, k, rows, :] = choose(kind, tables[2])
    weigh(lv, s, place)
    for t, src in enumerate((ui, uh)):
        for r, n in lv.chunks:
            rows = pl.ds(r, n)
            heat = pairs(src, 12, 0, lv, r, n)
            for k in range(NL):
                for c in (0, 1):
                    f = s["co"][t][c, 2, k, rows, :] * s["u"][t][c, k, rows, :]
                    if k == 0:
                        f = f + jnp.where(odd(n, k, c), heat[1], heat[0])
                    s["cf"][t][c, 6, k, rows, :] = s["iv"][t][c, k, rows, :] * f
    smooth(lv, s)
    restrict_rhs(lv, s, sr)
    for k in range(NL):
        for r in range(0, 64, 32):
            f5[k, pl.ds(r, 32), :] = sr[k, pl.ds(lv.base + r, 32), :]
    pack1(f5, 6, mf1, kf1, rr_f1)
    exf1 = exchange1(mf1, kf1, rr_f1, rf1, qf1, nf1)
    sides(exf1, s1f, "start")
    g3c[12] = b3c[...]
    absent1(rf1, qf1, nf1)

    arrive(exc1, s1c)
    unpack1(cu1, c1, 18, rc1, qc1, nc1)
    line("arrive", "gy", gy, ny, a5c, h5c, s5c)
    strip5(h5c, 18, d5c)
    l5c[at5] = d5c[...]
    for d in range(1, half):
        pltpu.make_async_remote_copy(
            src_ref=d5c, dst_ref=l5c.at[at5], send_sem=s6c.at[0], recv_sem=s6c.at[1],
            device_id={"gx": lax.rem(gx + 2 * d, nx)}, device_id_type=MESH,
        ).start()
    pack_coefficients(levels[1], st[1], c1, 0)
    weigh(levels[1], st[1], place)
    restrict_coefficients(levels[1], st[1], c1)
    pack_coefficients(levels[2], st[2], c1, levels[1].base + 2 * (8 - levels[2].base))
    weigh(levels[2], st[2], place)
    near("start", b3c, g3c, s3c)

    arrive(exf1, s1f)
    unpack1(f5, f1, 6, rf1, qf1, nf1)
    pack_rhs(levels[1], st[1], f1, 0)
    smooth(levels[1], st[1])
    restrict_rhs(levels[1], st[1], sr)
    pack_rhs(levels[2], st[2], sr, levels[1].base + 2 * (8 - levels[2].base))
    smooth(levels[2], st[2])
    restrict_rhs(levels[2], st[2], sr)
    for k in range(NL):
        f3[k, pl.ds(0, 16), :] = sr[k, pl.ds(levels[2].base, 16), :]
    pack3(f3, 1, b3f)
    near("arrive", b3c, g3c, s3c)
    near("start", b3f, g3f, s3f)
    strips = l5c.at[pl.ds(0, half - 1)]
    pltpu.make_async_copy(strips, strips, s6c.at[1]).wait()
    pltpu.make_async_copy(strips, strips, s6c.at[0]).wait()
    mine = l5c.at[pl.ds(core * half, half)]
    relay = pltpu.make_async_remote_copy(
        src_ref=mine, dst_ref=mine, send_sem=s7c.at[0], recv_sem=s7c.at[1],
        device_id={"gx": gx + 1 - 2 * core}, device_id_type=MESH,
    )
    relay.start()
    g3f[12] = b3f[...]
    unpack3(b3c, g3c, 3, c3)
    pack_coefficients(levels[3], st[3], c3, 0)
    weigh(levels[3], st[3], place)
    restrict_coefficients(levels[3], st[3], c1)
    pack_coefficients(levels[4], st[4], c1, levels[3].base + 2 * (8 - levels[4].base))
    weigh(levels[4], st[4], place)

    near("arrive", b3f, g3f, s3f)
    unpack3(b3f, g3f, 1, f3)
    pack_rhs(levels[3], st[3], f3, 0)
    smooth(levels[3], st[3])
    restrict_rhs(levels[3], st[3], sr)
    pack_rhs(levels[4], st[4], sr, levels[3].base + 2 * (8 - levels[4].base))
    smooth(levels[4], st[4])
    restrict_rhs(levels[4], st[4], sr)
    for k in range(NL):
        cu5[k, pl.ds(0, 8), :] = sr[k, pl.ds(levels[4].base, 8), :]
    pack5(cu5, 6, a5f)
    line("start", "gy", gy, ny, a5f, h5f, s5f)
    h5f[gy] = a5f[...]
    relay.wait_recv()

    whole5(l5c, 18, c5, lambda g: g % 2 * half + g // 2)
    pack_coefficients(levels[5], st[5], c5, 0)
    weigh(levels[5], st[5], place)
    line("arrive", "gy", gy, ny, a5f, h5f, s5f)
    strip5(h5f, 6, d5f)
    line("start", "gx", gx, nx, d5f, l5f, s6f)
    l5f[gx] = d5f[...]
    restrict_coefficients(levels[5], st[5], c1)
    pack_coefficients(levels[6], st[6], c1, 8)
    weigh(levels[6], st[6], place)
    sides(ex0, s0, "sent")
    sides(exc1, s1c, "sent")
    sides(exf1, s1f, "sent")
    near("sent", b3c, g3c, s3c)
    near("sent", b3f, g3f, s3f)
    line("sent", "gy", gy, ny, a5c, h5c, s5c)
    line("sent", "gy", gy, ny, a5f, h5f, s5f)
    relay.wait_send()
    line("arrive", "gx", gx, nx, d5f, l5f, s6f)
    whole5(l5f, 6, f5, lambda g: g)
    pack_rhs(levels[5], st[5], f5, 0)
    smooth(levels[5], st[5])
    restrict_rhs(levels[5], st[5], sr)
    pack_rhs(levels[6], st[6], sr, 8)
    coarse_solve(levels[6], st[6], cr, cp, cq, ce)

    spread(levels[6], st[6], sp)
    correct(levels[5], st[5], sp, 2 * levels[6].base + 8 - levels[5].base)
    smooth(levels[5], st[5])
    spread(levels[5], st[5], sp)
    lv, s = levels[4], st[4]
    first = 2 * levels[5].base + 8 - lv.base + 4 * gx
    for k in range(NL):
        x = sp[k, pl.ds(first, lv.rows), :]
        add = wide(pltpu.roll(x, lax.rem(128 - 4 * gy, 128), 1))
        for c in (0, 1):
            rows = pl.ds(8, lv.rows)
            s["u"][0][c, k, rows, :] = s["u"][0][c, k, rows, :] + add
    smooth(lv, s)
    for i in (3, 2, 1, 0):
        spread(levels[i + 1], st[i + 1], sp)
        correct(levels[i], st[i], sp, 2 * levels[i + 1].base + 8 - levels[i].base)
        smooth(levels[i], st[i])
    u = st[0]["u"][0]
    for k in range(NL):
        for r in range(0, 64, 32):
            red, black = u[0, k, pl.ds(levels[0].base + r, 32), :], u[1, k, pl.ds(levels[0].base + r, 32), :]
            m = odd(32, k, 0)
            out[k, pl.ds(2 * r, 32, stride=2), :] = jnp.where(m, black, red)
            out[k, pl.ds(2 * r + 1, 32, stride=2), :] = jnp.where(m, red, black)

    line("sent", "gx", gx, nx, d5f, l5f, s6f)


def solution(mesh):
    nx, ny = mesh.shape["gx"], mesh.shape["gy"]
    levels = [
        Level(0, 128, 12, 72, 8),
        Level(1, 64, 24, 64, 32),
        Level(2, 32, 16, 32, 16),
        Level(3, 16, 24, 40, 32),
        Level(4, 8, 16, 24, 16),
        Level(5, 4, 8, 2 * nx, 0, True),
        Level(6, 2, 8, max(8, nx), 0, True),
    ]

    def buffer(*shape):
        return pltpu.VMEM(shape, F32)

    scratch = []
    for lv in levels:
        tiles = 2 if lv.index == 0 else 1
        n = lv.total
        for shape in ((2, 6, n, 128), (2, 7, 6, n, 128), (2, 6, n, 128), (2, 6, n, 128), (2, 3, 6, n, 128)):
            scratch += [buffer(*shape)] * tiles
    scratch += [buffer(13, 144, 128)] * 2
    scratch += [buffer(18, n, 128) for n in (128, 64, 32, 16, 16, 8)]
    scratch += [buffer(6, 128, 128), buffer(6, 80, 128), buffer(6, max(64, 4 * nx), 128)]
    scratch += [buffer(18, 128, 128), buffer(18, 80, 128), buffer(18, 4 * nx, 128)]
    scratch += [buffer(6, 96, 128), buffer(6, 160, 128)]
    n = levels[6].total
    scratch += [buffer(2, 6, n, 128)] * 4
    scratch += [buffer(2, 13, 8, 128), buffer(4, 8, 128), buffer(2, 13, 8, 128), buffer(4, 8, 128)]
    for a in (18, 6):
        scratch += [buffer(2, a, 16, 128), buffer(4, a, 8, 128), buffer(2, a, 16, 128), buffer(4, a, 8, 128), buffer(2, a, 16, 128)]
    scratch += [buffer(2, 18, 16, 128), buffer(2, 6, 16, 128)]
    scratch += [buffer(3, 16, 128), buffer(25, 3, 16, 128), buffer(1, 16, 128), buffer(25, 1, 16, 128)]
    for rows in (40, 16):
        scratch += [buffer(8, 128), buffer(ny, 8, 128), buffer(rows, 128), buffer(nx, rows, 128)]
    scratch += [pltpu.SemaphoreType.DMA((2, 8))] * 3 + [pltpu.SemaphoreType.DMA((2,))] * 7

    def on_device(*args):
        vmem, smem = pl.BlockSpec(memory_space=pltpu.VMEM), pl.BlockSpec(memory_space=pltpu.SMEM)

        def body(*refs):
            kernel(nx, ny, levels, *refs)

        return pl.pallas_call(
            body,
            out_shape=jax.ShapeDtypeStruct((6, 128, 128), F32),
            in_specs=[vmem, vmem] + [smem] * 5,
            out_specs=vmem,
            scratch_shapes=scratch,
            compiler_params=pltpu.CompilerParams(
                collective_id=0, has_side_effects=True, vmem_limit_bytes=60 * 2**20
            ),
            name="vcycle",
        )(*args)

    placed = (P(None, "gx", "gy"), P(None, "gx", "gy"), P("gx", "gy"), P(), P(), P(), P())
    return jax.shard_map(on_device, mesh=mesh, in_specs=placed, out_specs=P(None, "gx", "gy"), check_vma=False)
```

```python
import jax
import jax.numpy as jnp
from jax import lax
from jax.experimental import pallas as pl
from jax.experimental.pallas import tpu as pltpu
from jax.sharding import PartitionSpec as P

MESH = pl.DeviceIdType.MESH
NL = 6
TILE = 16
ITERS = 12
F32 = jnp.float32


class Level:
    def __init__(self, index, block, base, rows, half, whole=False):
        self.index, self.block, self.base, self.rows, self.half, self.whole = index, block, base, rows, half, whole
        self.total = rows + 16
        self.scale = 0.25**index
        step = 24 if rows % 24 == 0 else 16 if rows % 16 == 0 else 8
        self.chunks = [(r, min(step, 8 + rows - r)) for r in range(8, 8 + rows, step)]


def lanes(n):
    return lax.broadcasted_iota(jnp.int32, (n, 128), 1)


def odd(n, k, c):
    bit = lanes(n) & 1
    return bit == 1 if (k + c) % 2 == 0 else bit == 0


def roll(x, shift):
    shift %= 128
    return x if shift == 0 else pltpu.roll(x, shift, 1)


def take(x, index):
    return jnp.take_along_axis(x, index, axis=1, mode="promise_in_bounds")


def thin(ref, spots):
    for a, r, n in spots:
        x = ref[a, pl.ds(r, n), :]
        ref[a, pl.ds(r, n), :] = 0.25 * (x + roll(x, 127))
    for a, r, n in spots:
        x = ref[a, pl.ds(r, n), :]
        ref[a, pl.ds(r, n), :] = take(x, (2 * lanes(n)) & 127)


def wide(x, split=64):
    j = lanes(x.shape[0])
    return take(x, jnp.where(j < split, j >> 1, 64 + (j >> 1)))


def around(refs, t, o, k, r, n, c, pick=()):
    ref = refs[t]
    here = ref[(o, *pick, k, pl.ds(r, n), slice(None))]
    before = ref[(o, *pick, k, pl.ds(r - 1, n), slice(None))]
    after = ref[(o, *pick, k, pl.ds(r + 1, n), slice(None))]
    far = jnp.where(odd(n, k, c), after, before)
    left, right = roll(here, 1), roll(here, 127)
    if len(refs) == 2:
        j = lanes(n)
        beside = refs[1 - t][(o, *pick, k, pl.ds(r, n), slice(None))]
        left = jnp.where(j == 0, roll(beside, 1), left)
        right = jnp.where(j == 127, roll(beside, 127), right)
    return here, far, left, right


def coupled(lv, s, t, c, k, r, n):
    o = 1 - c
    cf = s["cf"][t]
    here, far, left, right = around(s["u"], t, o, k, r, n, c)
    rows = pl.ds(r, n)
    a = cf[c, 0, k, rows, :] * here + cf[c, 1, k, rows, :] * far
    a = a + cf[c, 2, k, rows, :] * left + cf[c, 3, k, rows, :] * right
    if k > 0:
        a = a + cf[c, 4, k, rows, :] * s["u"][t][o, k - 1, rows, :]
    if k < NL - 1:
        a = a + cf[c, 5, k, rows, :] * s["u"][t][o, k + 1, rows, :]
    return a


def half_sweep(lv, s, c):
    for t in range(len(s["u"])):
        for k in range(NL):
            for r, n in lv.chunks:
                rows = pl.ds(r, n)
                f = s["cf"][t][c, 6, k, rows, :] + coupled(lv, s, t, c, k, r, n)
                s["u"][t][c, k, rows, :] = f * s["iv"][t][c, k, rows, :]


def smooth(lv, s):
    def sweep(i, _):
        half_sweep(lv, s, 0)
        half_sweep(lv, s, 1)
        return 0

    lax.fori_loop(0, 2, sweep, 0)


def residual(lv, s, t, k, r, n):
    rows = pl.ds(r, n)
    parts = []
    for c in (0, 1):
        image = s["dg"][t][c, k, rows, :] * s["u"][t][c, k, rows, :] - coupled(lv, s, t, c, k, r, n)
        parts.append(s["cf"][t][c, 6, k, rows, :] - image)
    return parts[0] + parts[1]


def inside(lv, t, r, n, gx, gy, nx, ny):
    row = lax.broadcasted_iota(jnp.int32, (n, 128), 0) + (r - lv.base)
    j = lanes(n)
    if lv.whole:
        return (row >= 0) & (row < lv.block * nx // 2) & (j < lv.block * ny)
    half = lv.half // 2
    if lv.index == 0:
        col = j if t == 0 else jnp.where(j < 64, j + 128, j - 128)
    elif lv.index == 1:
        col = jnp.where(j < 96, j, j - 128)
    else:
        col = jnp.where(j < 64, j, j - 128)
    ok = (row >= -half) & (row < lv.block // 2 + half) & (col >= -lv.half) & (col < lv.block + lv.half)
    row, col = row + gx * (lv.block // 2), col + gy * lv.block
    return ok & (row >= 0) & (row < lv.block * nx // 2) & (col >= 0) & (col < lv.block * ny)


def weigh(lv, s, place):
    h = 0.5 * lv.scale
    for t in range(len(s["u"])):
        co = s["co"]
        for r, n in lv.chunks:
            ok = inside(lv, t, r, n, *place)
            rows = pl.ds(r, n)
            for c in (0, 1):
                o = 1 - c
                for k in range(NL):
                    own = co[t][c, 0, k, rows, :]
                    ws = [h * (own + x) for x in around(co, t, o, k, r, n, c, (0,))]
                    m = odd(n, k, c)
                    diag = co[t][c, 2, k, rows, :] + jnp.where(m, ws[0], ws[1]) + jnp.where(m, ws[1], ws[0])
                    diag = diag + ws[2] + ws[3]
                    mine = co[t][c, 1, k, rows, :]
                    for other, there in ((k - 1, k > 0), (k + 1, k < NL - 1)):
                        if there:
                            face = 0.5 * (mine + co[t][o, 1, other, rows, :])
                            diag = diag + face
                            ws.append(face)
                        else:
                            ws.append(None)
                    inv = jnp.where(ok, 1.0 / diag, 0.0)
                    for i, w in enumerate(ws):
                        if w is not None:
                            s["cf"][t][c, i, k, rows, :] = w
                    s["dg"][t][c, k, rows, :] = diag
                    s["iv"][t][c, k, rows, :] = inv


def pairs(ref, a, start, lv, r, n):
    first = start + 2 * (r - 8)
    even = ref[a, pl.ds(first, n, stride=2), :]
    other = ref[a, pl.ds(first + 1, n, stride=2), :]
    return even, other


def pack_coefficients(lv, s, src, start):
    for m in range(3):
        for k in range(NL):
            for r, n in lv.chunks:
                even, other = pairs(src, m * NL + k, start, lv, r, n)
                for c in (0, 1):
                    s["co"][0][c, m, k, pl.ds(r, n), :] = jnp.where(odd(n, k, c), other, even)


def pack_rhs(lv, s, src, start):
    for k in range(NL):
        for r, n in lv.chunks:
            even, other = pairs(src, k, start, lv, r, n)
            rows = pl.ds(r, n)
            for c in (0, 1):
                f = jnp.where(odd(n, k, c), other, even)
                s["cf"][0][c, 6, k, rows, :] = f


def restrict_rhs(lv, s, dst):
    for k in range(NL):
        for r, n in lv.chunks:
            dst[k, pl.ds(r, n), :] = residual(lv, s, 0, k, r, n)
    thin(dst, [(k, r, n) for k in range(NL) for r, n in lv.chunks])


def restrict_coefficients(lv, s, dst):
    for m in range(3):
        for k in range(NL):
            for r, n in lv.chunks:
                rows = pl.ds(r, n)
                dst[m * NL + k, rows, :] = s["co"][0][0, m, k, rows, :] + s["co"][0][1, m, k, rows, :]
    thin(dst, [(a, r, n) for a in range(3 * NL) for r, n in lv.chunks])


def spread(lv, s, dst):
    for k in range(NL):
        for r, n in lv.chunks:
            red, black = s["u"][0][0, k, pl.ds(r, n), :], s["u"][0][1, k, pl.ds(r, n), :]
            m = odd(n, k, 0)
            dst[k, pl.ds(2 * r, n, stride=2), :] = jnp.where(m, black, red)
            dst[k, pl.ds(2 * r + 1, n, stride=2), :] = jnp.where(m, red, black)


def correct(lv, s, src, start):
    for k in range(NL):
        for r, n in lv.chunks:
            x = src[k, pl.ds(start + r - 8, n), :]
            rows = pl.ds(r, n)
            for t in range(len(s["u"])):
                if lv.index > 0:
                    add = wide(x, 96 if lv.index == 1 else 64)
                else:
                    j = lanes(n)
                    add = take(x, (j >> 1) + 64 * t)
                for c in (0, 1):
                    s["u"][t][c, k, rows, :] = s["u"][t][c, k, rows, :] + add


def choose(label, entries):
    b0, b1, b2 = (label & 1) == 1, (label & 2) == 2, (label & 4) == 4
    low = [jnp.where(b0, entries[i + 1], entries[i]) for i in (0, 2, 4, 6)]
    return jnp.where(b2, jnp.where(b1, low[3], low[2]), jnp.where(b1, low[1], low[0]))


def clear_margins(lv, s):
    for t in range(len(s["u"])):
        for r in (0, 8 + lv.rows):
            zero = jnp.zeros((8, 128), F32)
            for c in (0, 1):
                for k in range(NL):
                    s["u"][t][c, k, pl.ds(r, 8), :] = zero
                    s["co"][t][c, 0, k, pl.ds(r, 8), :] = zero


def clear(lv, s):
    for k in range(NL):
        for r, n in lv.chunks:
            for c in (0, 1):
                s["u"][0][c, k, pl.ds(r, n), :] = jnp.zeros((n, 128), F32)


def coarse_solve(lv, s, r_ref, p_ref, q_ref, e_ref):
    u, cf, dg, iv = s["u"][0], s["cf"][0], s["dg"][0], s["iv"][0]
    cells = [(c, k, r, n) for c in (0, 1) for k in range(NL) for r, n in lv.chunks]

    def total(parts):
        while len(parts) > 1:
            parts = [a + b for a, b in zip(parts[::2], parts[1::2])] + ([parts[-1]] if len(parts) % 2 else [])
        return jnp.sum(jnp.sum(parts[0], axis=0, keepdims=True), axis=1, keepdims=True)

    def images():
        ws, rz, zw = [], [], []
        for c, k, r, n in cells:
            rows = pl.ds(r, n)
            z = u[c, k, rows, :]
            w = dg[c, k, rows, :] * z - coupled(lv, s, 0, c, k, r, n)
            ws.append(w)
            rz.append(r_ref[c, k, rows, :] * z)
            zw.append(z * w)
        return ws, total(rz), total(zw)

    for c, k, r, n in cells:
        rows = pl.ds(r, n)
        f = cf[c, 6, k, rows, :]
        r_ref[c, k, rows, :] = f
        u[c, k, rows, :] = f * iv[c, k, rows, :]
    ws, rz, zw = images()
    for (c, k, r, n), w in zip(cells, ws):
        rows = pl.ds(r, n)
        p_ref[c, k, rows, :] = u[c, k, rows, :]
        q_ref[c, k, rows, :] = w
        e_ref[c, k, rows, :] = jnp.zeros_like(w)

    def step(i, carry):
        rz, alpha = carry
        for c, k, r, n in cells:
            rows = pl.ds(r, n)
            left = r_ref[c, k, rows, :] - alpha * q_ref[c, k, rows, :]
            r_ref[c, k, rows, :] = left
            u[c, k, rows, :] = left * iv[c, k, rows, :]
            e_ref[c, k, rows, :] = e_ref[c, k, rows, :] + alpha * p_ref[c, k, rows, :]
        ws, after, zw = images()
        beta = after / rz
        for (c, k, r, n), w in zip(cells, ws):
            rows = pl.ds(r, n)
            p_ref[c, k, rows, :] = u[c, k, rows, :] + beta * p_ref[c, k, rows, :]
            q_ref[c, k, rows, :] = w + beta * q_ref[c, k, rows, :]
        return after, after / (zw - beta * after / alpha)

    rz, alpha = lax.fori_loop(0, ITERS - 1, step, (rz, rz / zw))
    for c, k, r, n in cells:
        rows = pl.ds(r, n)
        u[c, k, rows, :] = e_ref[c, k, rows, :] + alpha * p_ref[c, k, rows, :]


def halve(src, dst, arrays, rows):
    step = min(rows, 32)
    spots = [(a, r, step) for a in range(arrays) for r in range(0, rows, step)]
    for a, r, n in spots:
        dst[a, pl.ds(r, n), :] = src[a, pl.ds(2 * r, n, stride=2), :] + src[a, pl.ds(2 * r + 1, n, stride=2), :]
    thin(dst, spots)


def kernel(nx, ny, levels, heat_field, substance, category, planar, vertical, mass, wattage, out, *scratch):
    gx, gy = lax.axis_index("gx"), lax.axis_index("gy")
    place = (gx, gy, nx, ny)
    half, core = nx // 2, lax.rem(gx, 2)
    at5 = core * half + gx // 2
    it = iter(scratch)
    st = []
    for lv in levels:
        tiles = 2 if lv.index == 0 else 1
        st.append({name: [next(it) for _ in range(tiles)] for name in ("u", "cf", "dg", "iv", "co")})
    ui, uh, cu0, cu1, cu2, cu3, cu4, cu5 = (next(it) for _ in range(8))
    f1, f3, f5, c1, c3, c5, sr, sp, cr, cp, cq, ce = (next(it) for _ in range(12))
    m0, k0, r0, q0 = (next(it) for _ in range(4))
    mc1, kc1, rc1, qc1, nc1 = (next(it) for _ in range(5))
    mf1, kf1, rf1, qf1, nf1 = (next(it) for _ in range(5))
    rr_c1, rr_f1 = next(it), next(it)
    b3c, g3c, b3f, g3f = (next(it) for _ in range(4))
    a5c, h5c, d5c, l5c = (next(it) for _ in range(4))
    a5f, h5f, d5f, l5f = (next(it) for _ in range(4))
    s0, s1c, s1f, s3c, s3f, s5c, s5f, s6c, s6f, s7c, s4c = (next(it) for _ in range(11))

    def exists(dx, dy):
        return (gx + dx >= 0) & (gx + dx < nx) & (gy + dy >= 0) & (gy + dy < ny)

    for q in range(25):
        if q != 12:
            g3c[q] = jnp.zeros(g3c.shape[1:], F32)
            g3f[q] = jnp.zeros(g3f.shape[1:], F32)
    barrier = pltpu.get_barrier_semaphore()

    def greet(**where):
        pl.semaphore_signal(barrier, inc=1, device_id=where, device_id_type=MESH)

    for dx in (-2, -1, 1, 2):
        for dy in (-2, -1, 1, 2):
            pl.when(exists(dx, dy))(lambda dx=dx, dy=dy: greet(gx=gx + dx, gy=gy + dy))
    for d in range(1, nx):
        greet(gx=lax.rem(gx + d, nx))
    for d in range(1, ny):
        greet(gy=lax.rem(gy + d, ny))

    def reach(at, size):
        return jnp.minimum(at, 2) + jnp.minimum(size - 1 - at, 2)

    for k in range(NL):
        for r in range(0, 128, 32):
            ui[k, pl.ds(8 + r, 32), :] = heat_field[k, pl.ds(r, 32), :]
            ui[NL + k, pl.ds(8 + r, 32), :] = substance[k, pl.ds(r, 32), :].astype(F32)
    for i in range(8):
        row = jnp.zeros((8, 128), F32)
        for jj in range(8):
            row = jnp.where((lanes(8) >> 4) == jj, wattage[category[i, jj]], row)
        ui[12, pl.ds(8 + 16 * i, 8), :] = row
        ui[12, pl.ds(16 + 16 * i, 8), :] = row

    for a in range(13):
        first, last = jnp.zeros((8, 128), F32), jnp.zeros((8, 128), F32)
        slot = lanes(8) >> 3
        for g in range(16):
            z = roll(ui[a, pl.ds(8 + 8 * g, 8), :], 8 * g)
            first = jnp.where(slot == g, z, first)
            last = jnp.where(slot == (g + 15) % 16, z, last)
        m0[0, a] = first
        m0[1, a] = last
    slot8 = lanes(8) >> 3
    for i, r in ((0, 8), (1, 128)):
        first, last = jnp.zeros((8, 128), F32), jnp.zeros((8, 128), F32)
        for a in range(13):
            z = roll(ui[a, pl.ds(r, 8), :], 8 * a)
            first = jnp.where(slot8 == a, z, first)
            last = jnp.where(slot8 == (a + 15) % 16, z, last)
        k0[2 * i] = first
        k0[2 * i + 1] = last

    tables = [[ref[i] for i in range(8)] for ref in (planar, vertical, mass)]

    def own(k, _):
        for r in range(0, 128, 16):
            label = substance[k, pl.ds(r, 16), :]
            for m in range(3):
                cu0[m * NL + k, pl.ds(r, 16), :] = choose(label, tables[m])
        return 0

    lax.fori_loop(0, NL, own, 0)
    cu4[...] = jnp.zeros(cu4.shape, F32)
    halve(cu0, cu1, 18, 64)

    pl.semaphore_wait(barrier, (nx - 1) + (ny - 1) + reach(gx, nx) * reach(gy, ny))

    SIDES = [(-1, 0), (1, 0), (0, -1), (0, 1), (-1, -1), (-1, 1), (1, -1), (1, 1)]

    def side_copy(i, src, dst, sems):
        dx, dy = SIDES[i]
        opposite = SIDES.index((-dx, -dy))
        return pltpu.make_async_remote_copy(
            src_ref=src, dst_ref=dst, send_sem=sems.at[0, i], recv_sem=sems.at[1, opposite],
            device_id={"gx": gx + dx, "gy": gy + dy}, device_id_type=MESH,
        )

    def sides(refs, sems, action):
        for i, (dx, dy) in enumerate(SIDES):
            @pl.when(exists(dx, dy))
            def _(i=i):
                copy = side_copy(i, refs[i][0], refs[i][1], sems)
                if action == "start":
                    copy.start()
                elif action == "sent":
                    copy.wait_send()

    def arrive(refs, sems):
        for i, (dx, dy) in enumerate(SIDES):
            opposite = SIDES.index((-dx, -dy))

            @pl.when(exists(dx, dy))
            def _(opposite=opposite):
                side_copy(opposite, refs[opposite][0], refs[opposite][1], sems).wait_recv()

    def absent(fills):
        for (dx, dy), ref in zip(SIDES, fills):
            @pl.when(jnp.logical_not(exists(dx, dy)))
            def _(ref=ref):
                ref[...] = jnp.zeros(ref.shape, F32)

    top, bottom = pl.ds(0, 8), pl.ds(136, 8)
    ex0 = [
        (ui.at[:, pl.ds(8, 8), :], ui.at[:, bottom, :]),
        (ui.at[:, pl.ds(128, 8), :], ui.at[:, top, :]),
        (m0.at[0], r0.at[1]),
        (m0.at[1], r0.at[0]),
        (k0.at[0], q0.at[3]),
        (k0.at[1], q0.at[2]),
        (k0.at[2], q0.at[1]),
        (k0.at[3], q0.at[0]),
    ]
    sides(ex0, s0, "start")
    absent([ui.at[:, top, :], ui.at[:, bottom, :], r0.at[0], r0.at[1], q0.at[0], q0.at[1], q0.at[2], q0.at[3]])

    def pack1(src, arrays, m, k, rws):
        slot = lanes(8) >> 5

        def one(i, _):
            for a, v in [(3 * i + e, v) for e in range(3) for v in range(2)]:
                first, last = jnp.zeros((8, 128), F32), jnp.zeros((8, 128), F32)
                for q in range(4):
                    z = roll(src[a, pl.ds(32 * v + 8 * q, 8), :], 32 * q)
                    first = jnp.where(slot == q, z, first)
                    last = jnp.where(slot == (q + 1) % 4, z, last)
                m[0, a, pl.ds(8 * v, 8), :] = first
                m[1, a, pl.ds(8 * v, 8), :] = last
                k[2 * v, a] = first
                k[2 * v + 1, a] = last
                x = src[a, pl.ds(32 * v, 16), :]
                y = src[a, pl.ds(32 * v + 16, 16), :]
                rws[v, a] = jnp.where(lanes(16) < 64, x, roll(y, 64))
            return 0

        lax.fori_loop(0, arrays // 3, one, 0)

    def exchange1(m, k, rws, r, q, n):
        return [
            (rws.at[0], n.at[1]), (rws.at[1], n.at[0]),
            (m.at[0], r.at[1]), (m.at[1], r.at[0]),
            (k.at[0], q.at[3]), (k.at[1], q.at[2]), (k.at[2], q.at[1]), (k.at[3], q.at[0]),
        ]

    def absent1(r, q, n):
        absent([n.at[0], n.at[1], r.at[0], r.at[1], q.at[0], q.at[1], q.at[2], q.at[3]])

    def unpack1(src, dst, arrays, r, q, n):
        slot, j8 = lanes(8) >> 5, lanes(8)

        def one(i, _):
            for a, v in [(3 * i + e, v) for e in range(3) for v in range(2)]:
                own_rows, over = n[v, a], roll(n[v, a], 64)
                for g in range(4):
                    z = roll(jnp.where(slot == g, q[2 * v + 1, a], q[2 * v, a]), 64 - 32 * g)
                    x = (own_rows if g < 2 else over)[8 * (g % 2) : 8 * (g % 2) + 8]
                    dst[a, pl.ds(96 * v + 8 * g, 8), :] = jnp.where(j8 < 64, x, z)
                    y = roll(jnp.where(slot == g, r[1, a, pl.ds(8 * v, 8), :], r[0, a, pl.ds(8 * v, 8), :]), 64 - 32 * g)
                    x = src[a, pl.ds(32 * v + 8 * g, 8), :]
                    dst[a, pl.ds(32 + 32 * v + 8 * g, 8), :] = jnp.where(j8 < 64, x, y)
            return 0

        lax.fori_loop(0, arrays // 3, one, 0)

    def pack3(src, sets, dst):
        for m in range(sets):
            total = src[m * NL, pl.ds(0, 16), :]
            for k in range(1, NL):
                z = roll(src[m * NL + k, pl.ds(0, 16), :], 16 * k)
                total = jnp.where((lanes(16) >> 4) == k, z, total)
            dst[m] = total

    def wait_for(at, size, part, sem):
        for n in (2, 3, 4):
            @pl.when(reach(at, size) == n)
            def _(n=n):
                pltpu.make_async_copy(part(n), part(n), sem).wait()

    def near(action, src, dst, sems):
        if action == "start":
            for q in [q for q in range(25) if q != 12]:
                dx, dy = q // 5 - 2, q % 5 - 2

                @pl.when(exists(dx, dy))
                def _(dx=dx, dy=dy, q=q):
                    pltpu.make_async_remote_copy(
                        src_ref=src, dst_ref=dst.at[24 - q], send_sem=sems.at[0], recv_sem=sems.at[1],
                        device_id={"gx": gx + dx, "gy": gy + dy}, device_id_type=MESH,
                    ).start()

            return
        for a in (2, 3, 4):
            for b in (2, 3, 4):
                @pl.when((reach(gx, nx) == a) & (reach(gy, ny) == b))
                def _(count=(a + 1) * (b + 1) - 1):
                    part = dst.at[pl.ds(0, count)]
                    pltpu.make_async_copy(part, part, sems.at[1 if action == "arrive" else 0]).wait()

    def unpack3(src, got, sets, dst):
        j = lanes(16)
        slot = j >> 4
        for m in range(sets):
            for x in range(5):
                for k in range(NL):
                    total = jnp.zeros((16, 128), F32)
                    for dy in range(-2, 3):
                        z = roll(got[x * 5 + dy + 2, m], 16 * dy - 16 * k)
                        total = jnp.where(slot == dy % 8, z, total)
                    dst[m * NL + k, pl.ds(16 * x, 16), :] = total

    def pack5(src, arrays, dst):
        total = src[0, pl.ds(0, 8), :]
        for a in range(1, arrays):
            total = jnp.where((lanes(8) >> 2) == a, roll(src[a, pl.ds(0, 8), :], 4 * a), total)
        dst[...] = total

    def line(action, axis, me, size, src, dst, sems):
        if action == "start":
            for d in range(1, size):
                pltpu.make_async_remote_copy(
                    src_ref=src, dst_ref=dst.at[me], send_sem=sems.at[0], recv_sem=sems.at[1],
                    device_id={axis: lax.rem(me + d, size)}, device_id_type=MESH,
                ).start()
            return
        part = dst.at[pl.ds(0, size - 1)]
        pltpu.make_async_copy(part, part, sems.at[1 if action == "arrive" else 0]).wait()

    def strip5(got, arrays, dst):
        j8 = lanes(8)
        low = lax.broadcasted_iota(jnp.int32, (8, 128), 0) < 4
        strips = []
        for a in range(arrays):
            total = jnp.zeros((8, 128), F32)
            for d in range(ny):
                total = jnp.where((j8 >> 2) == d, roll(got[d], 4 * d - 4 * a), total)
            strips.append(total)
        for t in range((arrays + 3) // 4):
            four = [strips[a] if a < arrays else jnp.zeros((8, 128), F32) for a in range(4 * t, 4 * t + 4)]
            x = jnp.where(j8 < 64, four[0], roll(four[1], 64))
            y = jnp.where(j8 < 64, four[2], roll(four[3], 64))
            dst[pl.ds(8 * t, 8), :] = jnp.where(low, x, pltpu.roll(y, 4, 0))

    def whole5(got, arrays, dst, order):
        j8 = lanes(8)
        low = lax.broadcasted_iota(jnp.int32, (8, 128), 0) < 4
        for a in range(arrays):
            t, up, right = a // 4, (a // 2) % 2, a % 2
            for h in range(nx // 2):
                x, y = got[order(2 * h), pl.ds(8 * t, 8), :], got[order(2 * h + 1), pl.ds(8 * t, 8), :]
                if up == 0:
                    y = pltpu.roll(y, 4, 0)
                else:
                    x = pltpu.roll(x, 4, 0)
                z = jnp.where(low, x, y)
                dst[a, pl.ds(8 * h, 8), :] = jnp.where(j8 < 64, roll(z, 64 * right), 0.0)

    exc1 = exchange1(mc1, kc1, rr_c1, rc1, qc1, nc1)
    pack1(cu1, 18, mc1, kc1, rr_c1)
    halve(cu1, cu2, 18, 32)
    sides(exc1, s1c, "start")
    halve(cu2, cu3, 18, 16)
    halve(cu3, cu4, 18, 8)
    halve(cu4, cu5, 18, 8)
    pack5(cu5, 18, a5c)
    pack3(cu3, 3, b3c)
    absent1(rc1, qc1, nc1)
    line("start", "gy", gy, ny, a5c, h5c, s5c)
    for dy in (-1, 1, -2, 2):
        @pl.when(exists(0, dy))
        def _(dy=dy):
            pltpu.make_async_remote_copy(
                src_ref=b3c, dst_ref=g3c.at[12 - dy], send_sem=s3c.at[0], recv_sem=s3c.at[1],
                device_id={"gy": gy + dy}, device_id_type=MESH,
            ).start()

    g3c[12] = b3c[...]
    h5c[gy] = a5c[...]

    for lv, s in zip(levels, st):
        clear_margins(lv, s)
    for lv, s in list(zip(levels, st))[1:6]:
        clear(lv, s)
    for k in range(NL):
        for r in (8, 80, 88):
            sp[k, pl.ds(r, 8), :] = jnp.zeros((8, 128), F32)

    lv, s = levels[0], st[0]

    def pack0(t, src, chunks):
        for r, n in chunks:
            ok = inside(lv, t, r, n, *place)
            rows = pl.ds(r, n)
            for k in range(NL):
                label = pairs(src, NL + k, 0, lv, r, n)
                value = pairs(src, k, 0, lv, r, n)
                for c in (0, 1):
                    m = odd(n, k, c)
                    kind = jnp.where(m, label[1], label[0]).astype(jnp.int32)
                    s["u"][t][c, k, rows, :] = jnp.where(m, value[1], value[0])
                    s["co"][t][c, 0, k, rows, :] = jnp.where(ok, choose(kind, tables[0]), 0.0)
                    s["co"][t][c, 1, k, rows, :] = choose(kind, tables[1])
                    s["co"][t][c, 2, k, rows, :] = choose(kind, tables[2])

    pack0(0, ui, [(16, 24), (40, 24), (64, 8)])
    arrive(ex0, s0)

    for a in range(13):
        for g in range(16):
            uh[a, pl.ds(8 + 8 * g, 8), :] = roll(jnp.where(slot8 == g, r0[1, a], r0[0, a]), -8 * g)
    for i, r in ((0, 0), (1, 136)):
        for a in range(13):
            uh[a, pl.ds(r, 8), :] = roll(jnp.where(slot8 == a, q0[2 * i + 1], q0[2 * i]), -8 * a)

    pack0(0, ui, [(8, 8), (72, 8)])
    pack0(1, uh, lv.chunks)
    weigh(lv, s, place)
    for t, src in enumerate((ui, uh)):
        for r, n in lv.chunks:
            rows = pl.ds(r, n)
            heat = pairs(src, 12, 0, lv, r, n)
            for k in range(NL):
                for c in (0, 1):
                    f = s["co"][t][c, 2, k, rows, :] * s["u"][t][c, k, rows, :]
                    if k == 0:
                        f = f + jnp.where(odd(n, k, c), heat[1], heat[0])
                    s["cf"][t][c, 6, k, rows, :] = f
    smooth(lv, s)
    restrict_rhs(lv, s, sr)
    for k in range(NL):
        for r in range(0, 64, 32):
            f5[k, pl.ds(r, 32), :] = sr[k, pl.ds(lv.base + r, 32), :]
    pack1(f5, 6, mf1, kf1, rr_f1)
    exf1 = exchange1(mf1, kf1, rr_f1, rf1, qf1, nf1)
    sides(exf1, s1f, "start")
    wait_for(gy, ny, lambda n: g3c.at[pl.ds(0, n)], s3c.at[1])
    for dx in (-1, 1, -2, 2):
        @pl.when(exists(dx, 0))
        def _(dx=dx):
            pltpu.make_async_remote_copy(
                src_ref=g3c.at[pl.ds(10, 5)], dst_ref=g3c.at[pl.ds(10 - 5 * dx, 5)], send_sem=s4c.at[0],
                recv_sem=s4c.at[1], device_id={"gx": gx + dx}, device_id_type=MESH,
            ).start()

    absent1(rf1, qf1, nf1)

    arrive(exc1, s1c)
    unpack1(cu1, c1, 18, rc1, qc1, nc1)
    line("arrive", "gy", gy, ny, a5c, h5c, s5c)
    strip5(h5c, 18, d5c)
    l5c[at5] = d5c[...]
    for d in range(1, half):
        pltpu.make_async_remote_copy(
            src_ref=d5c, dst_ref=l5c.at[at5], send_sem=s6c.at[0], recv_sem=s6c.at[1],
            device_id={"gx": lax.rem(gx + 2 * d, nx)}, device_id_type=MESH,
        ).start()
    pack_coefficients(levels[1], st[1], c1, 0)
    weigh(levels[1], st[1], place)
    restrict_coefficients(levels[1], st[1], c1)
    pack_coefficients(levels[2], st[2], c1, levels[1].base + 2 * (8 - levels[2].base))
    weigh(levels[2], st[2], place)

    arrive(exf1, s1f)
    unpack1(f5, f1, 6, rf1, qf1, nf1)
    pack_rhs(levels[1], st[1], f1, 0)
    smooth(levels[1], st[1])
    restrict_rhs(levels[1], st[1], sr)
    pack_rhs(levels[2], st[2], sr, levels[1].base + 2 * (8 - levels[2].base))
    smooth(levels[2], st[2])
    restrict_rhs(levels[2], st[2], sr)
    for k in range(NL):
        f3[k, pl.ds(0, 16), :] = sr[k, pl.ds(levels[2].base, 16), :]
    pack3(f3, 1, b3f)
    wait_for(gx, nx, lambda n: g3c.at[pl.ds(0, 5 * n)], s4c.at[1])
    near("start", b3f, g3f, s3f)
    strips = l5c.at[pl.ds(0, half - 1)]
    pltpu.make_async_copy(strips, strips, s6c.at[1]).wait()
    pltpu.make_async_copy(strips, strips, s6c.at[0]).wait()
    mine = l5c.at[pl.ds(core * half, half)]
    relay = pltpu.make_async_remote_copy(
        src_ref=mine, dst_ref=mine, send_sem=s7c.at[0], recv_sem=s7c.at[1],
        device_id={"gx": gx + 1 - 2 * core}, device_id_type=MESH,
    )
    relay.start()
    g3f[12] = b3f[...]
    unpack3(b3c, g3c, 3, c3)
    pack_coefficients(levels[3], st[3], c3, 0)
    weigh(levels[3], st[3], place)
    restrict_coefficients(levels[3], st[3], c1)
    pack_coefficients(levels[4], st[4], c1, levels[3].base + 2 * (8 - levels[4].base))
    weigh(levels[4], st[4], place)

    near("arrive", b3f, g3f, s3f)
    unpack3(b3f, g3f, 1, f3)
    pack_rhs(levels[3], st[3], f3, 0)
    smooth(levels[3], st[3])
    restrict_rhs(levels[3], st[3], sr)
    pack_rhs(levels[4], st[4], sr, levels[3].base + 2 * (8 - levels[4].base))
    smooth(levels[4], st[4])
    restrict_rhs(levels[4], st[4], sr)
    for k in range(NL):
        cu5[k, pl.ds(0, 8), :] = sr[k, pl.ds(levels[4].base, 8), :]
    pack5(cu5, 6, a5f)
    line("start", "gy", gy, ny, a5f, h5f, s5f)
    h5f[gy] = a5f[...]
    relay.wait_recv()

    whole5(l5c, 18, c5, lambda g: g % 2 * half + g // 2)
    pack_coefficients(levels[5], st[5], c5, 0)
    weigh(levels[5], st[5], place)
    line("arrive", "gy", gy, ny, a5f, h5f, s5f)
    strip5(h5f, 6, d5f)
    line("start", "gx", gx, nx, d5f, l5f, s6f)
    l5f[gx] = d5f[...]
    restrict_coefficients(levels[5], st[5], c1)
    pack_coefficients(levels[6], st[6], c1, 8)
    weigh(levels[6], st[6], place)
    sides(ex0, s0, "sent")
    sides(exc1, s1c, "sent")
    sides(exf1, s1f, "sent")
    wait_for(gy, ny, lambda n: g3c.at[pl.ds(0, n)], s3c.at[0])
    wait_for(gx, nx, lambda n: g3c.at[pl.ds(0, 5 * n)], s4c.at[0])
    near("sent", b3f, g3f, s3f)
    line("sent", "gy", gy, ny, a5c, h5c, s5c)
    line("sent", "gy", gy, ny, a5f, h5f, s5f)
    relay.wait_send()
    line("arrive", "gx", gx, nx, d5f, l5f, s6f)
    whole5(l5f, 6, f5, lambda g: g)
    pack_rhs(levels[5], st[5], f5, 0)
    smooth(levels[5], st[5])
    restrict_rhs(levels[5], st[5], sr)
    pack_rhs(levels[6], st[6], sr, 8)
    coarse_solve(levels[6], st[6], cr, cp, cq, ce)

    spread(levels[6], st[6], sp)
    correct(levels[5], st[5], sp, 2 * levels[6].base + 8 - levels[5].base)
    smooth(levels[5], st[5])
    spread(levels[5], st[5], sp)
    lv, s = levels[4], st[4]
    first = 2 * levels[5].base + 8 - lv.base + 4 * gx
    for k in range(NL):
        x = sp[k, pl.ds(first, lv.rows), :]
        add = wide(pltpu.roll(x, lax.rem(128 - 4 * gy, 128), 1))
        for c in (0, 1):
            rows = pl.ds(8, lv.rows)
            s["u"][0][c, k, rows, :] = s["u"][0][c, k, rows, :] + add
    smooth(lv, s)
    for i in (3, 2, 1, 0):
        spread(levels[i + 1], st[i + 1], sp)
        correct(levels[i], st[i], sp, 2 * levels[i + 1].base + 8 - levels[i].base)
        smooth(levels[i], st[i])
    u = st[0]["u"][0]
    for k in range(NL):
        for r in range(0, 64, 32):
            red, black = u[0, k, pl.ds(levels[0].base + r, 32), :], u[1, k, pl.ds(levels[0].base + r, 32), :]
            m = odd(32, k, 0)
            out[k, pl.ds(2 * r, 32, stride=2), :] = jnp.where(m, black, red)
            out[k, pl.ds(2 * r + 1, 32, stride=2), :] = jnp.where(m, red, black)

    line("sent", "gx", gx, nx, d5f, l5f, s6f)


def solution(mesh):
    nx, ny = mesh.shape["gx"], mesh.shape["gy"]
    levels = [
        Level(0, 128, 12, 72, 8),
        Level(1, 64, 24, 64, 32),
        Level(2, 32, 16, 32, 16),
        Level(3, 16, 24, 40, 32),
        Level(4, 8, 16, 24, 16),
        Level(5, 4, 8, 2 * nx, 0, True),
        Level(6, 2, 8, max(8, nx), 0, True),
    ]

    def buffer(*shape):
        return pltpu.VMEM(shape, F32)

    scratch = []
    for lv in levels:
        tiles = 2 if lv.index == 0 else 1
        n = lv.total
        for shape in ((2, 6, n, 128), (2, 7, 6, n, 128), (2, 6, n, 128), (2, 6, n, 128), (2, 3, 6, n, 128)):
            scratch += [buffer(*shape)] * tiles
    scratch += [buffer(13, 144, 128)] * 2
    scratch += [buffer(18, n, 128) for n in (128, 64, 32, 16, 16, 8)]
    scratch += [buffer(6, 128, 128), buffer(6, 80, 128), buffer(6, max(64, 4 * nx), 128)]
    scratch += [buffer(18, 128, 128), buffer(18, 80, 128), buffer(18, 4 * nx, 128)]
    scratch += [buffer(6, 96, 128), buffer(6, 160, 128)]
    n = levels[6].total
    scratch += [buffer(2, 6, n, 128)] * 4
    scratch += [buffer(2, 13, 8, 128), buffer(4, 8, 128), buffer(2, 13, 8, 128), buffer(4, 8, 128)]
    for a in (18, 6):
        scratch += [buffer(2, a, 16, 128), buffer(4, a, 8, 128), buffer(2, a, 16, 128), buffer(4, a, 8, 128), buffer(2, a, 16, 128)]
    scratch += [buffer(2, 18, 16, 128), buffer(2, 6, 16, 128)]
    scratch += [buffer(3, 16, 128), buffer(25, 3, 16, 128), buffer(1, 16, 128), buffer(25, 1, 16, 128)]
    for rows in (40, 16):
        scratch += [buffer(8, 128), buffer(ny, 8, 128), buffer(rows, 128), buffer(nx, rows, 128)]
    scratch += [pltpu.SemaphoreType.DMA((2, 8))] * 3 + [pltpu.SemaphoreType.DMA((2,))] * 8

    def on_device(*args):
        vmem, smem = pl.BlockSpec(memory_space=pltpu.VMEM), pl.BlockSpec(memory_space=pltpu.SMEM)

        def body(*refs):
            kernel(nx, ny, levels, *refs)

        return pl.pallas_call(
            body,
            out_shape=jax.ShapeDtypeStruct((6, 128, 128), F32),
            in_specs=[vmem, vmem] + [smem] * 5,
            out_specs=vmem,
            scratch_shapes=scratch,
            compiler_params=pltpu.CompilerParams(
                collective_id=0, has_side_effects=True, vmem_limit_bytes=60 * 2**20
            ),
            name="vcycle",
        )(*args)

    placed = (P(None, "gx", "gy"), P(None, "gx", "gy"), P("gx", "gy"), P(), P(), P(), P())
    return jax.shard_map(on_device, mesh=mesh, in_specs=placed, out_specs=P(None, "gx", "gy"), check_vma=False)
```

```python
import jax
import jax.numpy as jnp
from jax import lax
from jax.experimental import pallas as pl
from jax.experimental.pallas import tpu as pltpu
from jax.sharding import PartitionSpec as P

MESH = pl.DeviceIdType.MESH
NL = 6
TILE = 16
ITERS = 12
F32 = jnp.float32


class Level:
    def __init__(self, index, block, base, rows, half, whole=False):
        self.index, self.block, self.base, self.rows, self.half, self.whole = index, block, base, rows, half, whole
        self.total = rows + 16
        self.scale = 0.25**index
        step = 24 if rows % 24 == 0 else 16 if rows % 16 == 0 else 8
        self.chunks = [(r, min(step, 8 + rows - r)) for r in range(8, 8 + rows, step)]


def lanes(n):
    return lax.broadcasted_iota(jnp.int32, (n, 128), 1)


def odd(n, k, c):
    bit = lanes(n) & 1
    return bit == 1 if (k + c) % 2 == 0 else bit == 0


def roll(x, shift):
    shift %= 128
    return x if shift == 0 else pltpu.roll(x, shift, 1)


def take(x, index):
    return jnp.take_along_axis(x, index, axis=1, mode="promise_in_bounds")


def thin(ref, spots):
    for a, r, n in spots:
        x = ref[a, pl.ds(r, n), :]
        ref[a, pl.ds(r, n), :] = 0.25 * (x + roll(x, 127))
    for a, r, n in spots:
        x = ref[a, pl.ds(r, n), :]
        ref[a, pl.ds(r, n), :] = take(x, (2 * lanes(n)) & 127)


def wide(x, split=64):
    j = lanes(x.shape[0])
    return take(x, jnp.where(j < split, j >> 1, 64 + (j >> 1)))


def around(refs, t, o, k, r, n, c, pick=()):
    ref = refs[t]
    here = ref[(o, *pick, k, pl.ds(r, n), slice(None))]
    before = ref[(o, *pick, k, pl.ds(r - 1, n), slice(None))]
    after = ref[(o, *pick, k, pl.ds(r + 1, n), slice(None))]
    far = jnp.where(odd(n, k, c), after, before)
    left, right = roll(here, 1), roll(here, 127)
    if len(refs) == 2:
        j = lanes(n)
        beside = refs[1 - t][(o, *pick, k, pl.ds(r, n), slice(None))]
        left = jnp.where(j == 0, roll(beside, 1), left)
        right = jnp.where(j == 127, roll(beside, 127), right)
    return here, far, left, right


def coupled(lv, s, t, c, k, r, n):
    o = 1 - c
    cf = s["cf"][t]
    here, far, left, right = around(s["u"], t, o, k, r, n, c)
    rows = pl.ds(r, n)
    a = cf[c, 0, k, rows, :] * here + cf[c, 1, k, rows, :] * far
    a = a + cf[c, 2, k, rows, :] * left + cf[c, 3, k, rows, :] * right
    if k > 0:
        a = a + cf[c, 4, k, rows, :] * s["u"][t][o, k - 1, rows, :]
    if k < NL - 1:
        a = a + cf[c, 5, k, rows, :] * s["u"][t][o, k + 1, rows, :]
    return a


def half_sweep(lv, s, c, chunks):
    for t in range(len(s["u"])):
        for k in range(NL):
            for r, n in chunks:
                rows = pl.ds(r, n)
                f = s["cf"][t][c, 6, k, rows, :] + coupled(lv, s, t, c, k, r, n)
                s["u"][t][c, k, rows, :] = f * s["iv"][t][c, k, rows, :]


def smooth(lv, s, chunks=None):
    def sweep(i, _):
        half_sweep(lv, s, 0, chunks or lv.chunks)
        half_sweep(lv, s, 1, chunks or lv.chunks)
        return 0

    lax.fori_loop(0, 2, sweep, 0)


def residual(lv, s, t, k, r, n):
    rows = pl.ds(r, n)
    parts = []
    for c in (0, 1):
        image = s["dg"][t][c, k, rows, :] * s["u"][t][c, k, rows, :] - coupled(lv, s, t, c, k, r, n)
        parts.append(s["cf"][t][c, 6, k, rows, :] - image)
    return parts[0] + parts[1]


def inside(lv, t, r, n, gx, gy, nx, ny):
    row = lax.broadcasted_iota(jnp.int32, (n, 128), 0) + (r - lv.base)
    j = lanes(n)
    if lv.whole:
        return (row >= 0) & (row < lv.block * nx // 2) & (j < lv.block * ny)
    half = lv.half // 2
    if lv.index == 0:
        col = j if t == 0 else jnp.where(j < 64, j + 128, j - 128)
    elif lv.index == 1:
        col = jnp.where(j < 96, j, j - 128)
    else:
        col = jnp.where(j < 64, j, j - 128)
    ok = (row >= -half) & (row < lv.block // 2 + half) & (col >= -lv.half) & (col < lv.block + lv.half)
    row, col = row + gx * (lv.block // 2), col + gy * lv.block
    return ok & (row >= 0) & (row < lv.block * nx // 2) & (col >= 0) & (col < lv.block * ny)


def weigh(lv, s, place):
    h = 0.5 * lv.scale
    for t in range(len(s["u"])):
        co = s["co"]
        for r, n in lv.chunks:
            ok = inside(lv, t, r, n, *place)
            rows = pl.ds(r, n)
            for c in (0, 1):
                o = 1 - c
                for k in range(NL):
                    own = co[t][c, 0, k, rows, :]
                    ws = [h * (own + x) for x in around(co, t, o, k, r, n, c, (0,))]
                    m = odd(n, k, c)
                    diag = co[t][c, 2, k, rows, :] + jnp.where(m, ws[0], ws[1]) + jnp.where(m, ws[1], ws[0])
                    diag = diag + ws[2] + ws[3]
                    mine = co[t][c, 1, k, rows, :]
                    for other, there in ((k - 1, k > 0), (k + 1, k < NL - 1)):
                        if there:
                            face = 0.5 * (mine + co[t][o, 1, other, rows, :])
                            diag = diag + face
                            ws.append(face)
                        else:
                            ws.append(None)
                    inv = jnp.where(ok, 1.0 / diag, 0.0)
                    for i, w in enumerate(ws):
                        if w is not None:
                            s["cf"][t][c, i, k, rows, :] = w
                    s["dg"][t][c, k, rows, :] = diag
                    s["iv"][t][c, k, rows, :] = inv


def pairs(ref, a, start, lv, r, n):
    first = start + 2 * (r - 8)
    even = ref[a, pl.ds(first, n, stride=2), :]
    other = ref[a, pl.ds(first + 1, n, stride=2), :]
    return even, other


def pack_coefficients(lv, s, src, start):
    for m in range(3):
        for k in range(NL):
            for r, n in lv.chunks:
                even, other = pairs(src, m * NL + k, start, lv, r, n)
                for c in (0, 1):
                    s["co"][0][c, m, k, pl.ds(r, n), :] = jnp.where(odd(n, k, c), other, even)


def pack_rhs(lv, s, src, start):
    for k in range(NL):
        for r, n in lv.chunks:
            even, other = pairs(src, k, start, lv, r, n)
            rows = pl.ds(r, n)
            for c in (0, 1):
                f = jnp.where(odd(n, k, c), other, even)
                s["cf"][0][c, 6, k, rows, :] = f


def restrict_rhs(lv, s, dst):
    for k in range(NL):
        for r, n in lv.chunks:
            dst[k, pl.ds(r, n), :] = residual(lv, s, 0, k, r, n)
    thin(dst, [(k, r, n) for k in range(NL) for r, n in lv.chunks])


def restrict_coefficients(lv, s, dst):
    for m in range(3):
        for k in range(NL):
            for r, n in lv.chunks:
                rows = pl.ds(r, n)
                dst[m * NL + k, rows, :] = s["co"][0][0, m, k, rows, :] + s["co"][0][1, m, k, rows, :]
    thin(dst, [(a, r, n) for a in range(3 * NL) for r, n in lv.chunks])


def spread(lv, s, dst):
    for k in range(NL):
        for r, n in lv.chunks:
            red, black = s["u"][0][0, k, pl.ds(r, n), :], s["u"][0][1, k, pl.ds(r, n), :]
            m = odd(n, k, 0)
            dst[k, pl.ds(2 * r, n, stride=2), :] = jnp.where(m, black, red)
            dst[k, pl.ds(2 * r + 1, n, stride=2), :] = jnp.where(m, red, black)


def correct(lv, s, src, start, chunks=None):
    for k in range(NL):
        for r, n in chunks or lv.chunks:
            x = src[k, pl.ds(start + r - 8, n), :]
            rows = pl.ds(r, n)
            for t in range(len(s["u"])):
                if lv.index > 0:
                    add = wide(x, 96 if lv.index == 1 else 64)
                else:
                    j = lanes(n)
                    add = take(x, (j >> 1) + 64 * t)
                for c in (0, 1):
                    s["u"][t][c, k, rows, :] = s["u"][t][c, k, rows, :] + add


def choose(label, entries):
    b0, b1, b2 = (label & 1) == 1, (label & 2) == 2, (label & 4) == 4
    low = [jnp.where(b0, entries[i + 1], entries[i]) for i in (0, 2, 4, 6)]
    return jnp.where(b2, jnp.where(b1, low[3], low[2]), jnp.where(b1, low[1], low[0]))


def clear_margins(lv, s):
    for t in range(len(s["u"])):
        for r in (0, 8 + lv.rows):
            zero = jnp.zeros((8, 128), F32)
            for c in (0, 1):
                for k in range(NL):
                    s["u"][t][c, k, pl.ds(r, 8), :] = zero
                    s["co"][t][c, 0, k, pl.ds(r, 8), :] = zero


def clear(lv, s):
    for k in range(NL):
        for r, n in lv.chunks:
            for c in (0, 1):
                s["u"][0][c, k, pl.ds(r, n), :] = jnp.zeros((n, 128), F32)


def coarse_solve(lv, s, r_ref, p_ref, q_ref, e_ref):
    u, cf, dg, iv = s["u"][0], s["cf"][0], s["dg"][0], s["iv"][0]
    cells = [(c, k, r, n) for c in (0, 1) for k in range(NL) for r, n in lv.chunks]

    def total(parts):
        while len(parts) > 1:
            parts = [a + b for a, b in zip(parts[::2], parts[1::2])] + ([parts[-1]] if len(parts) % 2 else [])
        return jnp.sum(jnp.sum(parts[0], axis=0, keepdims=True), axis=1, keepdims=True)

    def images():
        ws, rz, zw = [], [], []
        for c, k, r, n in cells:
            rows = pl.ds(r, n)
            z = u[c, k, rows, :]
            w = dg[c, k, rows, :] * z - coupled(lv, s, 0, c, k, r, n)
            ws.append(w)
            rz.append(r_ref[c, k, rows, :] * z)
            zw.append(z * w)
        return ws, total(rz), total(zw)

    for c, k, r, n in cells:
        rows = pl.ds(r, n)
        f = cf[c, 6, k, rows, :]
        r_ref[c, k, rows, :] = f
        u[c, k, rows, :] = f * iv[c, k, rows, :]
    ws, rz, zw = images()
    for (c, k, r, n), w in zip(cells, ws):
        rows = pl.ds(r, n)
        p_ref[c, k, rows, :] = u[c, k, rows, :]
        q_ref[c, k, rows, :] = w
        e_ref[c, k, rows, :] = jnp.zeros_like(w)

    def step(i, carry):
        rz, alpha = carry
        for c, k, r, n in cells:
            rows = pl.ds(r, n)
            left = r_ref[c, k, rows, :] - alpha * q_ref[c, k, rows, :]
            r_ref[c, k, rows, :] = left
            u[c, k, rows, :] = left * iv[c, k, rows, :]
            e_ref[c, k, rows, :] = e_ref[c, k, rows, :] + alpha * p_ref[c, k, rows, :]
        ws, after, zw = images()
        beta = after / rz
        for (c, k, r, n), w in zip(cells, ws):
            rows = pl.ds(r, n)
            p_ref[c, k, rows, :] = u[c, k, rows, :] + beta * p_ref[c, k, rows, :]
            q_ref[c, k, rows, :] = w + beta * q_ref[c, k, rows, :]
        return after, after / (zw - beta * after / alpha)

    rz, alpha = lax.fori_loop(0, ITERS - 1, step, (rz, rz / zw))
    for c, k, r, n in cells:
        rows = pl.ds(r, n)
        u[c, k, rows, :] = e_ref[c, k, rows, :] + alpha * p_ref[c, k, rows, :]


def halve(src, dst, arrays, rows):
    step = min(rows, 32)
    spots = [(a, r, step) for a in range(arrays) for r in range(0, rows, step)]
    for a, r, n in spots:
        dst[a, pl.ds(r, n), :] = src[a, pl.ds(2 * r, n, stride=2), :] + src[a, pl.ds(2 * r + 1, n, stride=2), :]
    thin(dst, spots)


def kernel(nx, ny, levels, heat_field, substance, category, planar, vertical, mass, wattage, out, *scratch):
    gx, gy = lax.axis_index("gx"), lax.axis_index("gy")
    place = (gx, gy, nx, ny)
    half, core = nx // 2, lax.rem(gx, 2)
    at5 = core * half + gx // 2
    it = iter(scratch)
    st = []
    for lv in levels:
        tiles = 2 if lv.index == 0 else 1
        st.append({name: [next(it) for _ in range(tiles)] for name in ("u", "cf", "dg", "iv", "co")})
    ui, uh, cu0, cu1, cu2, cu3, cu4, cu5 = (next(it) for _ in range(8))
    f1, f3, f5, c1, c3, c5, sr, sp, cr, cp, cq, ce = (next(it) for _ in range(12))
    m0, k0, r0, q0 = (next(it) for _ in range(4))
    mc1, kc1, rc1, qc1, nc1 = (next(it) for _ in range(5))
    mf1, kf1, rf1, qf1, nf1 = (next(it) for _ in range(5))
    rr_c1, rr_f1 = next(it), next(it)
    b3c, g3c, b3f, g3f = (next(it) for _ in range(4))
    a5c, h5c, d5c, l5c = (next(it) for _ in range(4))
    a5f, h5f, d5f, l5f = (next(it) for _ in range(4))
    s0, s1c, s1f, s3c, s3f, s5c, s5f, s6c, s6f, s7c, s4c = (next(it) for _ in range(11))

    def exists(dx, dy):
        return (gx + dx >= 0) & (gx + dx < nx) & (gy + dy >= 0) & (gy + dy < ny)

    for q in range(25):
        if q != 12:
            g3c[q] = jnp.zeros(g3c.shape[1:], F32)
            g3f[q] = jnp.zeros(g3f.shape[1:], F32)
    barrier = pltpu.get_barrier_semaphore()

    def greet(**where):
        pl.semaphore_signal(barrier, inc=1, device_id=where, device_id_type=MESH)

    for dx in (-2, -1, 1, 2):
        for dy in (-2, -1, 1, 2):
            pl.when(exists(dx, dy))(lambda dx=dx, dy=dy: greet(gx=gx + dx, gy=gy + dy))
    for d in range(1, nx):
        greet(gx=lax.rem(gx + d, nx))
    for d in range(1, ny):
        greet(gy=lax.rem(gy + d, ny))

    def reach(at, size):
        return jnp.minimum(at, 2) + jnp.minimum(size - 1 - at, 2)

    for k in range(NL):
        for r in range(0, 128, 32):
            ui[k, pl.ds(8 + r, 32), :] = heat_field[k, pl.ds(r, 32), :]
            ui[NL + k, pl.ds(8 + r, 32), :] = substance[k, pl.ds(r, 32), :].astype(F32)
    for i in range(8):
        row = jnp.zeros((8, 128), F32)
        for jj in range(8):
            row = jnp.where((lanes(8) >> 4) == jj, wattage[category[i, jj]], row)
        ui[12, pl.ds(8 + 16 * i, 8), :] = row
        ui[12, pl.ds(16 + 16 * i, 8), :] = row

    for a in range(13):
        first, last = jnp.zeros((8, 128), F32), jnp.zeros((8, 128), F32)
        slot = lanes(8) >> 3
        for g in range(16):
            z = roll(ui[a, pl.ds(8 + 8 * g, 8), :], 8 * g)
            first = jnp.where(slot == g, z, first)
            last = jnp.where(slot == (g + 15) % 16, z, last)
        m0[0, a] = first
        m0[1, a] = last
    slot8 = lanes(8) >> 3
    for i, r in ((0, 8), (1, 128)):
        first, last = jnp.zeros((8, 128), F32), jnp.zeros((8, 128), F32)
        for a in range(13):
            z = roll(ui[a, pl.ds(r, 8), :], 8 * a)
            first = jnp.where(slot8 == a, z, first)
            last = jnp.where(slot8 == (a + 15) % 16, z, last)
        k0[2 * i] = first
        k0[2 * i + 1] = last

    tables = [[ref[i] for i in range(8)] for ref in (planar, vertical, mass)]

    def own(k, _):
        for r in range(0, 128, 16):
            label = substance[k, pl.ds(r, 16), :]
            for m in range(3):
                cu0[m * NL + k, pl.ds(r, 16), :] = choose(label, tables[m])
        return 0

    lax.fori_loop(0, NL, own, 0)
    cu4[...] = jnp.zeros(cu4.shape, F32)
    halve(cu0, cu1, 18, 64)

    pl.semaphore_wait(barrier, (nx - 1) + (ny - 1) + reach(gx, nx) * reach(gy, ny))

    SIDES = [(-1, 0), (1, 0), (0, -1), (0, 1), (-1, -1), (-1, 1), (1, -1), (1, 1)]

    def side_copy(i, src, dst, sems):
        dx, dy = SIDES[i]
        opposite = SIDES.index((-dx, -dy))
        return pltpu.make_async_remote_copy(
            src_ref=src, dst_ref=dst, send_sem=sems.at[0, i], recv_sem=sems.at[1, opposite],
            device_id={"gx": gx + dx, "gy": gy + dy}, device_id_type=MESH,
        )

    def sides(refs, sems, action):
        for i, (dx, dy) in enumerate(SIDES):
            @pl.when(exists(dx, dy))
            def _(i=i):
                copy = side_copy(i, refs[i][0], refs[i][1], sems)
                if action == "start":
                    copy.start()
                elif action == "sent":
                    copy.wait_send()

    def arrive(refs, sems):
        for i, (dx, dy) in enumerate(SIDES):
            opposite = SIDES.index((-dx, -dy))

            @pl.when(exists(dx, dy))
            def _(opposite=opposite):
                side_copy(opposite, refs[opposite][0], refs[opposite][1], sems).wait_recv()

    def absent(fills):
        for (dx, dy), ref in zip(SIDES, fills):
            @pl.when(jnp.logical_not(exists(dx, dy)))
            def _(ref=ref):
                ref[...] = jnp.zeros(ref.shape, F32)

    top, bottom = pl.ds(0, 8), pl.ds(136, 8)
    ex0 = [
        (ui.at[:, pl.ds(8, 8), :], ui.at[:, bottom, :]),
        (ui.at[:, pl.ds(128, 8), :], ui.at[:, top, :]),
        (m0.at[0], r0.at[1]),
        (m0.at[1], r0.at[0]),
        (k0.at[0], q0.at[3]),
        (k0.at[1], q0.at[2]),
        (k0.at[2], q0.at[1]),
        (k0.at[3], q0.at[0]),
    ]
    sides(ex0, s0, "start")
    absent([ui.at[:, top, :], ui.at[:, bottom, :], r0.at[0], r0.at[1], q0.at[0], q0.at[1], q0.at[2], q0.at[3]])

    def pack1(src, arrays, m, k, rws):
        slot = lanes(8) >> 5

        def one(i, _):
            for a, v in [(3 * i + e, v) for e in range(3) for v in range(2)]:
                first, last = jnp.zeros((8, 128), F32), jnp.zeros((8, 128), F32)
                for q in range(4):
                    z = roll(src[a, pl.ds(32 * v + 8 * q, 8), :], 32 * q)
                    first = jnp.where(slot == q, z, first)
                    last = jnp.where(slot == (q + 1) % 4, z, last)
                m[0, a, pl.ds(8 * v, 8), :] = first
                m[1, a, pl.ds(8 * v, 8), :] = last
                k[2 * v, a] = first
                k[2 * v + 1, a] = last
                x = src[a, pl.ds(32 * v, 16), :]
                y = src[a, pl.ds(32 * v + 16, 16), :]
                rws[v, a] = jnp.where(lanes(16) < 64, x, roll(y, 64))
            return 0

        lax.fori_loop(0, arrays // 3, one, 0)

    def exchange1(m, k, rws, r, q, n):
        return [
            (rws.at[0], n.at[1]), (rws.at[1], n.at[0]),
            (m.at[0], r.at[1]), (m.at[1], r.at[0]),
            (k.at[0], q.at[3]), (k.at[1], q.at[2]), (k.at[2], q.at[1]), (k.at[3], q.at[0]),
        ]

    def absent1(r, q, n):
        absent([n.at[0], n.at[1], r.at[0], r.at[1], q.at[0], q.at[1], q.at[2], q.at[3]])

    def unpack1(src, dst, arrays, r, q, n):
        slot, j8 = lanes(8) >> 5, lanes(8)

        def one(i, _):
            for a, v in [(3 * i + e, v) for e in range(3) for v in range(2)]:
                own_rows, over = n[v, a], roll(n[v, a], 64)
                for g in range(4):
                    z = roll(jnp.where(slot == g, q[2 * v + 1, a], q[2 * v, a]), 64 - 32 * g)
                    x = (own_rows if g < 2 else over)[8 * (g % 2) : 8 * (g % 2) + 8]
                    dst[a, pl.ds(96 * v + 8 * g, 8), :] = jnp.where(j8 < 64, x, z)
                    y = roll(jnp.where(slot == g, r[1, a, pl.ds(8 * v, 8), :], r[0, a, pl.ds(8 * v, 8), :]), 64 - 32 * g)
                    x = src[a, pl.ds(32 * v + 8 * g, 8), :]
                    dst[a, pl.ds(32 + 32 * v + 8 * g, 8), :] = jnp.where(j8 < 64, x, y)
            return 0

        lax.fori_loop(0, arrays // 3, one, 0)

    def pack3(src, sets, dst):
        for m in range(sets):
            total = src[m * NL, pl.ds(0, 16), :]
            for k in range(1, NL):
                z = roll(src[m * NL + k, pl.ds(0, 16), :], 16 * k)
                total = jnp.where((lanes(16) >> 4) == k, z, total)
            dst[m] = total

    def wait_for(at, size, part, sem):
        for n in (2, 3, 4):
            @pl.when(reach(at, size) == n)
            def _(n=n):
                pltpu.make_async_copy(part(n), part(n), sem).wait()

    def near(action, src, dst, sems):
        if action == "start":
            for q in [q for q in range(25) if q != 12]:
                dx, dy = q // 5 - 2, q % 5 - 2

                @pl.when(exists(dx, dy))
                def _(dx=dx, dy=dy, q=q):
                    pltpu.make_async_remote_copy(
                        src_ref=src, dst_ref=dst.at[24 - q], send_sem=sems.at[0], recv_sem=sems.at[1],
                        device_id={"gx": gx + dx, "gy": gy + dy}, device_id_type=MESH,
                    ).start()

            return
        for a in (2, 3, 4):
            for b in (2, 3, 4):
                @pl.when((reach(gx, nx) == a) & (reach(gy, ny) == b))
                def _(count=(a + 1) * (b + 1) - 1):
                    part = dst.at[pl.ds(0, count)]
                    pltpu.make_async_copy(part, part, sems.at[1 if action == "arrive" else 0]).wait()

    def unpack3(src, got, sets, dst):
        j = lanes(16)
        slot = j >> 4
        for m in range(sets):
            for x in range(5):
                for k in range(NL):
                    total = jnp.zeros((16, 128), F32)
                    for dy in range(-2, 3):
                        z = roll(got[x * 5 + dy + 2, m], 16 * dy - 16 * k)
                        total = jnp.where(slot == dy % 8, z, total)
                    dst[m * NL + k, pl.ds(16 * x, 16), :] = total

    def pack5(src, arrays, dst):
        total = src[0, pl.ds(0, 8), :]
        for a in range(1, arrays):
            total = jnp.where((lanes(8) >> 2) == a, roll(src[a, pl.ds(0, 8), :], 4 * a), total)
        dst[...] = total

    def line(action, axis, me, size, src, dst, sems):
        if action == "start":
            for d in range(1, size):
                pltpu.make_async_remote_copy(
                    src_ref=src, dst_ref=dst.at[me], send_sem=sems.at[0], recv_sem=sems.at[1],
                    device_id={axis: lax.rem(me + d, size)}, device_id_type=MESH,
                ).start()
            return
        part = dst.at[pl.ds(0, size - 1)]
        pltpu.make_async_copy(part, part, sems.at[1 if action == "arrive" else 0]).wait()

    def strip5(got, arrays, dst):
        j8 = lanes(8)
        low = lax.broadcasted_iota(jnp.int32, (8, 128), 0) < 4
        strips = []
        for a in range(arrays):
            total = jnp.zeros((8, 128), F32)
            for d in range(ny):
                total = jnp.where((j8 >> 2) == d, roll(got[d], 4 * d - 4 * a), total)
            strips.append(total)
        for t in range((arrays + 3) // 4):
            four = [strips[a] if a < arrays else jnp.zeros((8, 128), F32) for a in range(4 * t, 4 * t + 4)]
            x = jnp.where(j8 < 64, four[0], roll(four[1], 64))
            y = jnp.where(j8 < 64, four[2], roll(four[3], 64))
            dst[pl.ds(8 * t, 8), :] = jnp.where(low, x, pltpu.roll(y, 4, 0))

    def whole5(got, arrays, dst, order):
        j8 = lanes(8)
        low = lax.broadcasted_iota(jnp.int32, (8, 128), 0) < 4
        for a in range(arrays):
            t, up, right = a // 4, (a // 2) % 2, a % 2
            for h in range(nx // 2):
                x, y = got[order(2 * h), pl.ds(8 * t, 8), :], got[order(2 * h + 1), pl.ds(8 * t, 8), :]
                if up == 0:
                    y = pltpu.roll(y, 4, 0)
                else:
                    x = pltpu.roll(x, 4, 0)
                z = jnp.where(low, x, y)
                dst[a, pl.ds(8 * h, 8), :] = jnp.where(j8 < 64, roll(z, 64 * right), 0.0)

    exc1 = exchange1(mc1, kc1, rr_c1, rc1, qc1, nc1)
    pack1(cu1, 18, mc1, kc1, rr_c1)
    halve(cu1, cu2, 18, 32)
    sides(exc1, s1c, "start")
    halve(cu2, cu3, 18, 16)
    halve(cu3, cu4, 18, 8)
    halve(cu4, cu5, 18, 8)
    pack5(cu5, 18, a5c)
    pack3(cu3, 3, b3c)
    absent1(rc1, qc1, nc1)
    line("start", "gy", gy, ny, a5c, h5c, s5c)
    for dy in (-1, 1, -2, 2):
        @pl.when(exists(0, dy))
        def _(dy=dy):
            pltpu.make_async_remote_copy(
                src_ref=b3c, dst_ref=g3c.at[12 - dy], send_sem=s3c.at[0], recv_sem=s3c.at[1],
                device_id={"gy": gy + dy}, device_id_type=MESH,
            ).start()

    g3c[12] = b3c[...]
    h5c[gy] = a5c[...]

    for lv, s in zip(levels, st):
        clear_margins(lv, s)
    for lv, s in list(zip(levels, st))[1:6]:
        clear(lv, s)
    for k in range(NL):
        for r in (8, 80, 88):
            sp[k, pl.ds(r, 8), :] = jnp.zeros((8, 128), F32)

    lv, s = levels[0], st[0]

    def pack0(t, src, chunks):
        for r, n in chunks:
            ok = inside(lv, t, r, n, *place)
            rows = pl.ds(r, n)
            for k in range(NL):
                label = pairs(src, NL + k, 0, lv, r, n)
                value = pairs(src, k, 0, lv, r, n)
                for c in (0, 1):
                    m = odd(n, k, c)
                    kind = jnp.where(m, label[1], label[0]).astype(jnp.int32)
                    s["u"][t][c, k, rows, :] = jnp.where(m, value[1], value[0])
                    s["co"][t][c, 0, k, rows, :] = jnp.where(ok, choose(kind, tables[0]), 0.0)
                    s["co"][t][c, 1, k, rows, :] = choose(kind, tables[1])
                    s["co"][t][c, 2, k, rows, :] = choose(kind, tables[2])

    pack0(0, ui, [(16, 24), (40, 24), (64, 8)])
    arrive(ex0, s0)

    for a in range(13):
        for g in range(16):
            uh[a, pl.ds(8 + 8 * g, 8), :] = roll(jnp.where(slot8 == g, r0[1, a], r0[0, a]), -8 * g)
    for i, r in ((0, 0), (1, 136)):
        for a in range(13):
            uh[a, pl.ds(r, 8), :] = roll(jnp.where(slot8 == a, q0[2 * i + 1], q0[2 * i]), -8 * a)

    pack0(0, ui, [(8, 8), (72, 8)])
    pack0(1, uh, lv.chunks)
    weigh(lv, s, place)
    for t, src in enumerate((ui, uh)):
        for r, n in lv.chunks:
            rows = pl.ds(r, n)
            heat = pairs(src, 12, 0, lv, r, n)
            for k in range(NL):
                for c in (0, 1):
                    f = s["co"][t][c, 2, k, rows, :] * s["u"][t][c, k, rows, :]
                    if k == 0:
                        f = f + jnp.where(odd(n, k, c), heat[1], heat[0])
                    s["cf"][t][c, 6, k, rows, :] = f
    smooth(lv, s)
    restrict_rhs(lv, s, sr)
    for k in range(NL):
        for r in range(0, 64, 32):
            f5[k, pl.ds(r, 32), :] = sr[k, pl.ds(lv.base + r, 32), :]
    pack1(f5, 6, mf1, kf1, rr_f1)
    exf1 = exchange1(mf1, kf1, rr_f1, rf1, qf1, nf1)
    sides(exf1, s1f, "start")
    wait_for(gy, ny, lambda n: g3c.at[pl.ds(0, n)], s3c.at[1])
    for dx in (-1, 1, -2, 2):
        @pl.when(exists(dx, 0))
        def _(dx=dx):
            pltpu.make_async_remote_copy(
                src_ref=g3c.at[pl.ds(10, 5)], dst_ref=g3c.at[pl.ds(10 - 5 * dx, 5)], send_sem=s4c.at[0],
                recv_sem=s4c.at[1], device_id={"gx": gx + dx}, device_id_type=MESH,
            ).start()

    absent1(rf1, qf1, nf1)

    arrive(exc1, s1c)
    unpack1(cu1, c1, 18, rc1, qc1, nc1)
    line("arrive", "gy", gy, ny, a5c, h5c, s5c)
    strip5(h5c, 18, d5c)
    l5c[at5] = d5c[...]
    for d in range(1, half):
        pltpu.make_async_remote_copy(
            src_ref=d5c, dst_ref=l5c.at[at5], send_sem=s6c.at[0], recv_sem=s6c.at[1],
            device_id={"gx": lax.rem(gx + 2 * d, nx)}, device_id_type=MESH,
        ).start()
    pack_coefficients(levels[1], st[1], c1, 0)
    weigh(levels[1], st[1], place)
    restrict_coefficients(levels[1], st[1], c1)
    pack_coefficients(levels[2], st[2], c1, levels[1].base + 2 * (8 - levels[2].base))
    weigh(levels[2], st[2], place)

    arrive(exf1, s1f)
    unpack1(f5, f1, 6, rf1, qf1, nf1)
    pack_rhs(levels[1], st[1], f1, 0)
    smooth(levels[1], st[1])
    restrict_rhs(levels[1], st[1], sr)
    pack_rhs(levels[2], st[2], sr, levels[1].base + 2 * (8 - levels[2].base))
    smooth(levels[2], st[2])
    restrict_rhs(levels[2], st[2], sr)
    for k in range(NL):
        f3[k, pl.ds(0, 16), :] = sr[k, pl.ds(levels[2].base, 16), :]
    pack3(f3, 1, b3f)
    sides(ex0, s0, "sent")
    near("start", b3f, g3f, s3f)
    g3f[12] = b3f[...]
    wait_for(gx, nx, lambda n: g3c.at[pl.ds(0, 5 * n)], s4c.at[1])
    unpack3(b3c, g3c, 3, c3)
    pack_coefficients(levels[3], st[3], c3, 0)
    weigh(levels[3], st[3], place)
    restrict_coefficients(levels[3], st[3], c1)
    pack_coefficients(levels[4], st[4], c1, levels[3].base + 2 * (8 - levels[4].base))
    weigh(levels[4], st[4], place)

    near("arrive", b3f, g3f, s3f)
    strips = l5c.at[pl.ds(0, half - 1)]
    pltpu.make_async_copy(strips, strips, s6c.at[1]).wait()
    mine = l5c.at[pl.ds(core * half, half)]
    relay = pltpu.make_async_remote_copy(
        src_ref=mine, dst_ref=mine, send_sem=s7c.at[0], recv_sem=s7c.at[1],
        device_id={"gx": gx + 1 - 2 * core}, device_id_type=MESH,
    )
    relay.start()
    unpack3(b3f, g3f, 1, f3)
    pack_rhs(levels[3], st[3], f3, 0)
    smooth(levels[3], st[3])
    restrict_rhs(levels[3], st[3], sr)
    pack_rhs(levels[4], st[4], sr, levels[3].base + 2 * (8 - levels[4].base))
    smooth(levels[4], st[4])
    restrict_rhs(levels[4], st[4], sr)
    for k in range(NL):
        cu5[k, pl.ds(0, 8), :] = sr[k, pl.ds(levels[4].base, 8), :]
    pack5(cu5, 6, a5f)
    sides(exc1, s1c, "sent")
    line("start", "gy", gy, ny, a5f, h5f, s5f)
    h5f[gy] = a5f[...]
    relay.wait_recv()

    whole5(l5c, 18, c5, lambda g: g % 2 * half + g // 2)
    pack_coefficients(levels[5], st[5], c5, 0)
    weigh(levels[5], st[5], place)
    line("arrive", "gy", gy, ny, a5f, h5f, s5f)
    strip5(h5f, 6, d5f)
    sides(exf1, s1f, "sent")
    line("start", "gx", gx, nx, d5f, l5f, s6f)
    l5f[gx] = d5f[...]
    restrict_coefficients(levels[5], st[5], c1)
    pack_coefficients(levels[6], st[6], c1, 8)
    weigh(levels[6], st[6], place)
    pltpu.make_async_copy(strips, strips, s6c.at[0]).wait()
    wait_for(gy, ny, lambda n: g3c.at[pl.ds(0, n)], s3c.at[0])
    wait_for(gx, nx, lambda n: g3c.at[pl.ds(0, 5 * n)], s4c.at[0])
    near("sent", b3f, g3f, s3f)
    line("sent", "gy", gy, ny, a5c, h5c, s5c)
    line("sent", "gy", gy, ny, a5f, h5f, s5f)
    relay.wait_send()
    line("arrive", "gx", gx, nx, d5f, l5f, s6f)
    whole5(l5f, 6, f5, lambda g: g)
    pack_rhs(levels[5], st[5], f5, 0)
    smooth(levels[5], st[5])
    restrict_rhs(levels[5], st[5], sr)
    pack_rhs(levels[6], st[6], sr, 8)
    coarse_solve(levels[6], st[6], cr, cp, cq, ce)

    spread(levels[6], st[6], sp)
    correct(levels[5], st[5], sp, 2 * levels[6].base + 8 - levels[5].base)
    smooth(levels[5], st[5])
    spread(levels[5], st[5], sp)
    lv, s = levels[4], st[4]
    first = 2 * levels[5].base + 8 - lv.base + 4 * gx
    for k in range(NL):
        x = sp[k, pl.ds(first, lv.rows), :]
        add = wide(pltpu.roll(x, lax.rem(128 - 4 * gy, 128), 1))
        for c in (0, 1):
            rows = pl.ds(8, lv.rows)
            s["u"][0][c, k, rows, :] = s["u"][0][c, k, rows, :] + add
    smooth(lv, s, [(8, 16)])
    for i in (3, 2, 1, 0):
        rows = {3: [(16, 24)], 1: [(16, 24), (40, 24)]}.get(i)
        spread(levels[i + 1], st[i + 1], sp)
        correct(levels[i], st[i], sp, 2 * levels[i + 1].base + 8 - levels[i].base, rows)
        smooth(levels[i], st[i], rows)
    u = st[0]["u"][0]
    for k in range(NL):
        for r in range(0, 64, 32):
            red, black = u[0, k, pl.ds(levels[0].base + r, 32), :], u[1, k, pl.ds(levels[0].base + r, 32), :]
            m = odd(32, k, 0)
            out[k, pl.ds(2 * r, 32, stride=2), :] = jnp.where(m, black, red)
            out[k, pl.ds(2 * r + 1, 32, stride=2), :] = jnp.where(m, red, black)

    line("sent", "gx", gx, nx, d5f, l5f, s6f)


def solution(mesh):
    nx, ny = mesh.shape["gx"], mesh.shape["gy"]
    levels = [
        Level(0, 128, 12, 72, 8),
        Level(1, 64, 24, 64, 32),
        Level(2, 32, 16, 32, 16),
        Level(3, 16, 24, 40, 32),
        Level(4, 8, 16, 24, 16),
        Level(5, 4, 8, 2 * nx, 0, True),
        Level(6, 2, 8, max(8, nx), 0, True),
    ]

    def buffer(*shape):
        return pltpu.VMEM(shape, F32)

    scratch = []
    for lv in levels:
        tiles = 2 if lv.index == 0 else 1
        n = lv.total
        for shape in ((2, 6, n, 128), (2, 7, 6, n, 128), (2, 6, n, 128), (2, 6, n, 128), (2, 3, 6, n, 128)):
            scratch += [buffer(*shape)] * tiles
    scratch += [buffer(13, 144, 128)] * 2
    scratch += [buffer(18, n, 128) for n in (128, 64, 32, 16, 16, 8)]
    scratch += [buffer(6, 128, 128), buffer(6, 80, 128), buffer(6, max(64, 4 * nx), 128)]
    scratch += [buffer(18, 128, 128), buffer(18, 80, 128), buffer(18, 4 * nx, 128)]
    scratch += [buffer(6, 96, 128), buffer(6, 160, 128)]
    n = levels[6].total
    scratch += [buffer(2, 6, n, 128)] * 4
    scratch += [buffer(2, 13, 8, 128), buffer(4, 8, 128), buffer(2, 13, 8, 128), buffer(4, 8, 128)]
    for a in (18, 6):
        scratch += [buffer(2, a, 16, 128), buffer(4, a, 8, 128), buffer(2, a, 16, 128), buffer(4, a, 8, 128), buffer(2, a, 16, 128)]
    scratch += [buffer(2, 18, 16, 128), buffer(2, 6, 16, 128)]
    scratch += [buffer(3, 16, 128), buffer(25, 3, 16, 128), buffer(1, 16, 128), buffer(25, 1, 16, 128)]
    for rows in (40, 16):
        scratch += [buffer(8, 128), buffer(ny, 8, 128), buffer(rows, 128), buffer(nx, rows, 128)]
    scratch += [pltpu.SemaphoreType.DMA((2, 8))] * 3 + [pltpu.SemaphoreType.DMA((2,))] * 8

    def on_device(*args):
        vmem, smem = pl.BlockSpec(memory_space=pltpu.VMEM), pl.BlockSpec(memory_space=pltpu.SMEM)

        def body(*refs):
            kernel(nx, ny, levels, *refs)

        return pl.pallas_call(
            body,
            out_shape=jax.ShapeDtypeStruct((6, 128, 128), F32),
            in_specs=[vmem, vmem] + [smem] * 5,
            out_specs=vmem,
            scratch_shapes=scratch,
            compiler_params=pltpu.CompilerParams(
                collective_id=0, has_side_effects=True, vmem_limit_bytes=60 * 2**20
            ),
            name="vcycle",
        )(*args)

    placed = (P(None, "gx", "gy"), P(None, "gx", "gy"), P("gx", "gy"), P(), P(), P(), P())
    return jax.shard_map(on_device, mesh=mesh, in_specs=placed, out_specs=P(None, "gx", "gy"), check_vma=False)
```
